128 devices in a mesh: row: 8 (over x_hi, y), col: 16 (over z, x_lo, core).
Axes of the slice: x: 4 (x_hi: 2, x_lo: 2; x = x_hi * 2 + x_lo), y: 4, z: 4, core: 2. Of those that a mesh axis runs over, the one named last changes fastest.
Arguments:
- velocity: float32 [3, 16, 16, 36, 32, 512], P(None, 'col', 'row'), may hold values from -6 to 6
- y_sizes: int32 [16], replicated, may hold values from 1 to 36, 512 in all
- old_place: int32 [16, 16], replicated, may hold values from 0 to 15, each once within a row
- new_col: int32 [16, 16], replicated, may hold values from 0 to 15, each once within a row
Outputs:
- divergence: float32 [16, 16, 2, 512, 512], P('row', 'col')
- peak: float32 [512, 512], replicated
The draws below stay inside these ranges and needn't reach their ends.
Inputs may be any that keep to these rules, and one draw needn't show every extreme that they name: `y_sizes`: the heights sum to 512 and the tallest is exactly 36. `old_place`: each row is a permutation of 0 to 15. `new_col`: each row is a permutation of 0 to 16 - 1.
All inputs are finite; a program needn't handle non-finite values.
Results may differ from the reference program's by a relative error of at most 0.0003.
Values sent between devices are 32-bit elements; how exact they have to be, the bound alone decides.
A program may use at most 320 MiB of HBM per device.

```python
import math
import jax
import jax.numpy as jnp
import numpy as np
from jax import lax

NX = 512
ZB = 32
YCAP = 36
NBZ = 16
NBY = 16
NY = 512
N_COL = 16


def block_levels(own_key, dims, pieces, low, top_value):
    def one(axis_at, blocks):
        heights = jax.random.uniform(jax.random.fold_in(jax.random.fold_in(own_key, 6), axis_at), (blocks,), jnp.float32, low / len(pieces), top_value / len(pieces))
        return jnp.repeat(jnp.exp(heights), dims[axis_at] // blocks).reshape((-1,) + (1,) * (len(dims) - axis_at - 1))

    gain = one(*pieces[0])
    for cut in pieces[1:]:
        gain = gain * one(*cut)
    return gain


def split_up(amount, total, limit, slope):
    portions = [(1 << 20) // math.isqrt(grade ** slope) + 1 for grade in range(2, amount + 1)]
    rest, given = total - limit - (amount - 1), [1] * (amount - 1)
    while rest > 0:
        candidates = [i for i in range(amount - 1) if given[i] < limit]
        mass, budget = sum([portions[i] for i in candidates]), rest
        for i in candidates:
            more = min(limit - given[i], max(1, budget * portions[i] // mass), rest)
            given[i] = given[i] + more
            rest = rest - more
    return np.array([limit] + given)


def ragged_sizes(key, amount, total, most, slope):
    if amount == 2:
        one = jax.random.randint(key, (), max(1, total - most), min(most, total - 1) + 1)
        return jnp.stack([one, total - one])
    sizes = jnp.asarray(split_up(amount, total, most, slope), jnp.int32)
    twos = (amount - 1) // 2
    donor, receiver = sizes[1:1 + 2 * twos:2], sizes[2:2 + 2 * twos:2]
    slack = jnp.minimum(donor - 1, most - receiver)
    moved = jax.random.randint(jax.random.fold_in(key, 1), (twos,), 0, 1 << 20) % (slack + 1)
    sizes = sizes.at[1:1 + 2 * twos:2].set(donor - moved).at[2:2 + 2 * twos:2].set(receiver + moved)
    return sizes[jax.random.permutation(jax.random.fold_in(key, 2), amount)]


def normal_values(stream_key, extent, scale, most, cuts=(), kind=jnp.bfloat16):
    loudness = block_levels(stream_key, extent, cuts, -0.22, 0.18) if cuts else 1.0
    drawn = jax.random.normal(stream_key, extent, jnp.float32) * scale * loudness
    return jnp.minimum(jnp.maximum(drawn, -most), most).astype(kind)


def setup_inputs(seed: int = 0) -> dict:
    key_of = jax.random.split(jax.random.key(seed), 5)
    velocity = normal_values(key_of[0], (3, NBZ, NBY, YCAP, ZB, NX), 1.0, 6.0, ((1, 16), (2, 8)), jnp.float32)
    y_sizes = ragged_sizes(key_of[1], NBY, NY, YCAP, 1).astype(jnp.int32)
    old_place = jax.vmap(lambda own: jax.random.permutation(own, NBY))(jax.random.split(key_of[2], NBZ)).reshape((NBZ, NBY)).astype(jnp.int32)
    new_col = jax.vmap(lambda own: jax.random.permutation(own, N_COL))(jax.random.split(key_of[3], NBZ)).reshape((NBZ, N_COL)).astype(jnp.int32)
    return {"velocity": velocity, "y_sizes": y_sizes, "old_place": old_place, "new_col": new_col}


def derive(field, axis):
    count = field.shape[axis]
    spectrum = jnp.fft.rfft(field, axis=axis)
    modes = jnp.arange(count // 2 + 1)
    wave = jnp.where(modes == count // 2, 0, modes).astype(field.dtype) * (4.0 / count)
    shape = [1] * field.ndim
    shape[axis] = count // 2 + 1
    spectrum = spectrum * (1j * wave.reshape(shape))
    return jnp.fft.irfft(spectrum, n=count, axis=axis).astype(field.dtype)


def source_rows(y_sizes, old_place, row_depth, height):
    ends = jnp.cumsum(y_sizes).astype(jnp.int32)
    starts = (ends - y_sizes).astype(jnp.int32)
    cells = jnp.arange(height, dtype=jnp.int32)
    block = jnp.sum((cells[:, None] >= ends[None, :]).astype(jnp.int32), axis=1).astype(jnp.int32)
    offset = cells - jnp.take(starts, block)
    return (jnp.take(old_place, block, axis=1) * row_depth + offset).astype(jnp.int32)


def assemble(pair):
    block, index = pair
    flat = block.reshape(-1, block.shape[2], block.shape[3])
    return jnp.transpose(jnp.take(flat, index, axis=0), (1, 0, 2))


def reference(velocity, y_sizes, old_place, new_col):
    row_depth = velocity.shape[3]
    rows = source_rows(y_sizes, old_place, row_depth, NY)
    vertical = lax.map(assemble, (velocity[2], rows)).reshape(-1, NY, NX)
    slope_z = derive(vertical, 0).reshape(N_COL, ZB, NY, NX)

    def combine(group):
        block_x, block_y, index, part_z = group
        slope_x = derive(assemble((block_x, index)), 2)
        slope_y = derive(assemble((block_y, index)), 1)
        return slope_x + slope_y + part_z

    field = lax.map(combine, (velocity[0], velocity[1], rows, slope_z))
    peak = jnp.max(jnp.abs(field), axis=(0, 1))
    field = field.reshape(N_COL, N_COL, ZB // N_COL, NY, NX)
    hits = (new_col[:, :, None] == jnp.arange(N_COL, dtype=jnp.int32)[None, None, :]).astype(jnp.int32)
    slab_of = jnp.sum(hits * jnp.arange(N_COL, dtype=jnp.int32)[None, :, None], axis=1).astype(jnp.int32)
    divergence = jnp.take_along_axis(field, slab_of[:, :, None, None, None], axis=1)
    return (divergence, peak)
```

```python
import functools
import math

import jax
import jax.numpy as jnp
import numpy as np
from jax import lax
from jax.experimental import pallas as pl
from jax.experimental.pallas import tpu as pltpu
from jax.sharding import PartitionSpec as P

BOTH = ("row", "col")


def spectral_matrix(count):
    gap = (np.arange(count)[:, None] - np.arange(count)[None, :]) % count
    angle = gap.astype(np.float64) * (math.pi / count)
    parity = 1.0 - 2.0 * (gap % 2)
    divisor = np.where(gap == 0, 1.0, np.sin(angle))
    return np.where(gap == 0, 0.0, parity * np.cos(angle) / divisor * (2.0 / count))


def two_halves(matrix):
    high = matrix.astype(np.float32).astype(jnp.bfloat16)
    low = (matrix - high.astype(np.float64)).astype(np.float32).astype(jnp.bfloat16)
    return jnp.asarray(high), jnp.asarray(low)


def split(value):
    high = value.astype(jnp.bfloat16)
    return high, (value - high.astype(jnp.float32)).astype(jnp.bfloat16)


def dot(a, b):
    return jnp.dot(a, b, preferred_element_type=jnp.float32)


def prepare_kernel(v_ref, high_ref, low_ref, out_ref):
    rows, planes, width = v_ref.shape[1:]
    parts = out_ref.shape[0]
    flat = out_ref.reshape(parts * rows, out_ref.shape[2])

    def emit(piece):
        for row in range(rows):
            value = piece(row)
            stacked = jnp.concatenate(
                [value[:, q * parts : (q + 1) * parts] for q in range(width // parts)], axis=0
            )
            flat[pl.ds(row, parts, stride=rows), :] = stacked.T

    @pl.when(pl.program_id(0) == 0)
    def _():
        high, low = split(v_ref[0].reshape(rows * planes, width))
        slope = dot(high, high_ref[...]) + (dot(high, low_ref[...]) + dot(low, high_ref[...]))
        emit(lambda row: slope[row * planes : (row + 1) * planes])

    @pl.when(pl.program_id(0) != 0)
    def _():
        emit(lambda row: v_ref[0, row])


def prepare(velocity, high, low, parts):
    fields, rows, planes, width = velocity.shape
    lanes = planes * width // parts
    groups = rows // 8
    whole = pl.BlockSpec((width, width), lambda f, g: (0, 0))
    return pl.pallas_call(
        prepare_kernel,
        grid=(fields, groups),
        in_specs=[pl.BlockSpec((1, 8, planes, width), lambda f, g: (f, g, 0, 0)), whole, whole],
        out_specs=pl.BlockSpec((parts, 8, lanes), lambda f, g: (0, f * groups + g, 0)),
        out_shape=jax.ShapeDtypeStruct((parts, fields * rows, lanes), jnp.float32),
        compiler_params=pltpu.CompilerParams(vmem_limit_bytes=48 << 20),
        cost_estimate=pl.CostEstimate(
            flops=6 * rows * planes * width * width,
            bytes_accessed=8 * fields * rows * planes * width,
            transcendentals=0,
        ),
        name="prepare",
    )(velocity, high, low)


def middle_kernel(
    sizes_ref, place_ref, col_ref, r_ref, high_ref, low_ref, out_ref,
    aligned, v_high, v_low, total, field, peaks,
):
    step = pl.program_id(0)
    blocks = place_ref.shape[1]
    depth = r_ref.shape[2] // 6
    height = field.shape[1]
    zblocks = place_ref.shape[0]
    planes = field.shape[0] // zblocks
    quarters = total.shape[0]
    lanes = r_ref.shape[3]
    chunks = height // lanes

    @pl.when(step < zblocks)
    def _():
        start = 0
        for b in range(blocks):
            place = place_ref[step, b]
            for f in range(3):
                aligned[f, pl.ds(start, depth), :] = r_ref[
                    place // 2, 0, pl.ds(2 * depth * f + depth * (place % 2), depth), :
                ]
            start = start + sizes_ref[b]
        high, low = split(aligned[1, :height, :])
        slope = dot(high_ref[...], high) + (dot(low_ref[...], high) + dot(high_ref[...], low))
        slope = (slope + aligned[0, :height, :]).T
        vertical = aligned[2, :height, :].T
        high, low = split(vertical)
        at = pl.multiple_of(step * planes, planes)
        for q in range(quarters):
            rows = slice(q * planes, (q + 1) * planes)
            total[q, pl.ds(at, planes), :] = slope[rows]
            v_high[q, pl.ds(at, planes), :] = high[rows]
            v_low[q, pl.ds(at, planes), :] = low[rows]

    @pl.when((step >= zblocks) & (step < zblocks + quarters))
    def _():
        q = step - zblocks
        value = total[q] + (
            dot(high_ref[...], v_high[q])
            + (dot(low_ref[...], v_high[q]) + dot(high_ref[...], v_low[q]))
        )
        field[...] = value
        top = jnp.max(jnp.abs(value), axis=0, keepdims=True)
        for chunk in range(chunks):
            peaks[pl.ds(q * chunks + chunk, 1), :] = top[:, chunk * lanes : (chunk + 1) * lanes]
        slabs = col_ref.shape[1]
        for zblock in range(zblocks):
            for slab in range(slabs):
                target = (zblock // 2) * slabs + col_ref[zblock, slab]
                low_row = zblock * planes + 2 * slab
                for chunk in range(chunks):
                    at = 4 * chunk + 2 * (zblock % 2)
                    out_ref[target, at : at + 2, :] = field[
                        low_row : low_row + 2, chunk * lanes : (chunk + 1) * lanes
                    ]

    @pl.when(step == zblocks + quarters)
    def _():
        out_ref[...] = jnp.broadcast_to(peaks[...][None], out_ref.shape)


def middle(received, sizes, old_place, new_col, high, low):
    rows, cols, depth, lanes = received.shape
    zblocks = old_place.shape[0]
    height = high.shape[0]
    parts = rows * cols
    quarters = 4
    whole = pl.BlockSpec(high.shape, lambda i: (0, 0))
    smem = pl.BlockSpec(memory_space=pltpu.SMEM)
    return pl.pallas_call(
        middle_kernel,
        grid=(zblocks + quarters + 1,),
        in_specs=[
            smem,
            smem,
            smem,
            pl.BlockSpec(
                (rows, 1, depth, lanes), lambda i: (0, jnp.minimum(i, zblocks - 1), 0, 0)
            ),
            whole,
            whole,
        ],
        out_specs=pl.BlockSpec(
            (parts, 16, lanes), lambda i: (0, jnp.maximum(i - zblocks, 0), 0)
        ),
        out_shape=jax.ShapeDtypeStruct((parts, 16 * (quarters + 1), lanes), jnp.float32),
        scratch_shapes=[
            pltpu.VMEM((3, height + 40, lanes), jnp.float32),
            pltpu.VMEM((quarters, height, height), jnp.bfloat16),
            pltpu.VMEM((quarters, height, height), jnp.bfloat16),
            pltpu.VMEM((quarters, height, height), jnp.float32),
            pltpu.VMEM((height, height), jnp.float32),
            pltpu.VMEM((16, lanes), jnp.float32),
        ],
        compiler_params=pltpu.CompilerParams(vmem_limit_bytes=56 << 20),
        cost_estimate=pl.CostEstimate(
            flops=48 * height**3, bytes_accessed=20 << 20, transcendentals=0
        ),
        name="middle",
    )(sizes, old_place, new_col, received, high, low)


def finish_kernel(g_ref, p_ref, out_ref, peak_ref):
    parts, rows, lanes = g_ref.shape
    flat = g_ref.reshape(parts * rows, lanes)
    tops = p_ref.reshape(parts * rows, lanes)
    thick = out_ref.shape[0]
    chunks = rows // thick
    q = pl.program_id(0)
    for chunk in range(chunks):
        ys = slice(chunk * lanes, (chunk + 1) * lanes)
        for plane in range(thick):
            out_ref[plane, ys, :] = flat[pl.ds(chunk * thick + plane, parts, stride=rows), :].T
        peak_ref[ys, :] = tops[pl.ds(q * chunks + chunk, parts, stride=rows), :].T


def finish(received, thick, height):
    parts, rows, lanes = received.shape
    quarters = rows // 16 - 1
    return pl.pallas_call(
        finish_kernel,
        grid=(quarters,),
        in_specs=[
            pl.BlockSpec((parts, 16, lanes), lambda q: (0, q, 0)),
            pl.BlockSpec((parts, 16, lanes), lambda q: (0, quarters, 0)),
        ],
        out_specs=[
            pl.BlockSpec((thick, height, parts), lambda q: (0, 0, q)),
            pl.BlockSpec((height, parts), lambda q: (0, q)),
        ],
        out_shape=[
            jax.ShapeDtypeStruct((thick, height, quarters * parts), jnp.float32),
            jax.ShapeDtypeStruct((height, quarters * parts), jnp.float32),
        ],
        compiler_params=pltpu.CompilerParams(vmem_limit_bytes=48 << 20),
        cost_estimate=pl.CostEstimate(flops=1 << 20, bytes_accessed=10 << 20, transcendentals=0),
        name="finish",
    )(received, received)


def exchange(blocks):
    return lax.all_to_all(blocks, BOTH, split_axis=0, concat_axis=0, tiled=True)


def on_device(velocity, y_sizes, old_place, new_col):
    fields, _, places, depth, planes, width = velocity.shape
    rows, cols = lax.axis_size("row"), lax.axis_size("col")
    parts = rows * cols
    matrix = spectral_matrix(width)
    high, low = two_halves(matrix)
    high_t, low_t = two_halves(matrix.T)
    outgoing = prepare(
        velocity.reshape(fields, places * depth, planes, width), high_t, low_t, parts
    )
    arrived = exchange(outgoing).reshape(rows, cols, fields * places * depth, parts)
    shares = middle(arrived, y_sizes, old_place, new_col, high, low)
    field, peak = finish(exchange(shares), 4, width)
    return field.reshape(2, 1, 2, width, width), peak


def solution(mesh):
    in_specs = (P(None, "col", "row", None, None, None), P(), P(), P())
    out_specs = (P("row", "col", None, None, None), P())
    return jax.shard_map(
        on_device, mesh=mesh, in_specs=in_specs, out_specs=out_specs, check_vma=False
    )
```

```python
import functools
import math

import jax
import jax.numpy as jnp
import numpy as np
from jax import lax
from jax.experimental import pallas as pl
from jax.experimental.pallas import tpu as pltpu
from jax.sharding import PartitionSpec as P

BOTH = ("row", "col")


def spectral_matrix(count):
    gap = (np.arange(count)[:, None] - np.arange(count)[None, :]) % count
    angle = gap.astype(np.float64) * (math.pi / count)
    parity = 1.0 - 2.0 * (gap % 2)
    divisor = np.where(gap == 0, 1.0, np.sin(angle))
    return np.where(gap == 0, 0.0, parity * np.cos(angle) / divisor * (2.0 / count))


def two_halves(matrix):
    high = matrix.astype(np.float32).astype(jnp.bfloat16)
    low = (matrix - high.astype(np.float64)).astype(np.float32).astype(jnp.bfloat16)
    return jnp.asarray(high), jnp.asarray(low)


def split(value):
    high = value.astype(jnp.bfloat16)
    return high, (value - high.astype(jnp.float32)).astype(jnp.bfloat16)


def dot(a, b):
    return jnp.dot(a, b, preferred_element_type=jnp.float32)


def spread_kernel(
    v_ref, high_ref, low_ref, out_ref, stage, send, in_sems, send_sem, recv_sem, own_sem
):
    fields, rows, planes, width = v_ref.shape
    parts, _, lanes = out_ref.shape
    chunk = send.shape[1] // parts
    per_field = rows // 8
    groups = fields * per_field
    per_chunk = chunk // 8
    slots = stage.shape[0]
    row, col = lax.axis_index("row"), lax.axis_index("col")
    me = row * 16 + col
    x, y, z, core = (row // 4) * 2 + (col // 2) % 2, row % 4, col // 4, col % 2

    def load(n):
        return pltpu.make_async_copy(
            v_ref.at[fields - 1 - n // per_field, pl.ds((n % per_field) * 8, 8)],
            stage.at[n % slots],
            in_sems.at[n % slots],
        )

    def post(j):
        at = pl.ds(pl.multiple_of(j * chunk, 8), chunk)

        def one(i, _):
            offset = ((i + core * (parts - 2 * i)) * 37) % parts
            there_x = (x + offset // 32) % 4
            there_y = (y + (offset // 8) % 4) % 4
            there_z = (z + (offset // 2) % 4) % 4
            there_core = (core + offset % 2) % 2
            to_row = (there_x // 2) * 4 + there_y
            to_col = there_z * 4 + (there_x % 2) * 2 + there_core
            part = to_row * 16 + to_col
            pltpu.make_async_remote_copy(
                src_ref=send.at[j, pl.ds(pl.multiple_of(part * chunk, 8), chunk)],
                dst_ref=out_ref.at[me, at],
                send_sem=send_sem,
                recv_sem=recv_sem,
                device_id=(to_row, to_col),
                device_id_type=pl.DeviceIdType.MESH,
            ).start()
            return 0

        lax.fori_loop(1, parts, one, 0)
        pltpu.make_async_copy(
            send.at[j, pl.ds(pl.multiple_of(me * chunk, 8), chunk)], out_ref.at[me, at], own_sem
        ).start()

    def group(n, slope_of):
        load(n).wait()
        value = slope_of(stage.at[n % slots])
        for r in range(8):
            piece = value(r)
            stacked = jnp.concatenate(
                [piece[:, q * parts : (q + 1) * parts] for q in range(width // parts)], axis=0
            )
            at = pl.ds((n % per_chunk) * 8 + r, parts, stride=chunk)
            send[n // per_chunk, at, :] = stacked.T

        @pl.when(n + slots < groups)
        def _():
            load(n + slots).start()

        @pl.when((n % per_chunk == 0) & (n > 0))
        def _():
            post(n // per_chunk - 1)

        return 0

    def plain(ref):
        return lambda r: ref[r]

    def along_x(ref):
        high, low = split(ref[...].reshape(8 * planes, width))
        slope = dot(high, high_ref[...]) + (dot(high, low_ref[...]) + dot(low, high_ref[...]))
        return lambda r: slope[r * planes : (r + 1) * planes]

    for n in range(slots):
        load(n).start()
    middle = (fields - 1) * per_field
    lax.fori_loop(0, middle, lambda n, _: group(n, plain), 0)
    lax.fori_loop(middle, groups, lambda n, _: group(n, along_x), 0)
    post(groups // per_chunk - 1)
    sent = out_ref.at[pl.ds(0, parts - 1)]
    pltpu.make_async_copy(out_ref.at[me], out_ref.at[me], own_sem).wait()
    pltpu.make_async_copy(sent, sent, send_sem).wait()
    pltpu.make_async_copy(sent, sent, recv_sem).wait()


def spread(velocity, high, low, parts):
    fields, rows, planes, width = velocity.shape
    lanes = planes * width // parts
    chunk = 24
    vmem = pl.BlockSpec(memory_space=pltpu.VMEM)
    anywhere = pl.BlockSpec(memory_space=pl.ANY)
    return pl.pallas_call(
        spread_kernel,
        in_specs=[anywhere, vmem, vmem],
        out_specs=anywhere,
        out_shape=jax.ShapeDtypeStruct((parts, fields * rows, lanes), jnp.float32),
        scratch_shapes=[
            pltpu.VMEM((3, 8, planes, width), jnp.float32),
            pltpu.VMEM((fields * rows // chunk, parts * chunk, lanes), jnp.float32),
            pltpu.SemaphoreType.DMA((3,)),
            pltpu.SemaphoreType.DMA,
            pltpu.SemaphoreType.DMA,
            pltpu.SemaphoreType.DMA,
        ],
        compiler_params=pltpu.CompilerParams(vmem_limit_bytes=48 << 20, has_side_effects=True),
        cost_estimate=pl.CostEstimate(
            flops=6 * rows * planes * width * width,
            bytes_accessed=8 * fields * rows * planes * width,
            transcendentals=0,
        ),
        name="spread",
    )(velocity, high, low)


def middle_kernel(
    sizes_ref, place_ref, col_ref, r_ref, high_ref, low_ref, out_ref,
    aligned, v_high, v_low, total, field, peaks,
):
    step = pl.program_id(0)
    blocks = place_ref.shape[1]
    depth = r_ref.shape[2] // 6
    height = field.shape[1]
    zblocks = place_ref.shape[0]
    planes = field.shape[0] // zblocks
    quarters = total.shape[0]
    lanes = r_ref.shape[3]
    chunks = height // lanes

    @pl.when(step < zblocks)
    def _():
        start = 0
        for b in range(blocks):
            place = place_ref[step, b]
            for f in range(3):
                aligned[f, pl.ds(start, depth), :] = r_ref[
                    place // 2, 0, pl.ds(2 * depth * f + depth * (place % 2), depth), :
                ]
            start = start + sizes_ref[b]
        high, low = split(aligned[1, :height, :])
        slope = dot(high_ref[...], high) + (dot(low_ref[...], high) + dot(high_ref[...], low))
        slope = (slope + aligned[2, :height, :]).T
        vertical = aligned[0, :height, :].T
        high, low = split(vertical)
        at = pl.multiple_of(step * planes, planes)
        for q in range(quarters):
            rows = slice(q * planes, (q + 1) * planes)
            total[q, pl.ds(at, planes), :] = slope[rows]
            v_high[q, pl.ds(at, planes), :] = high[rows]
            v_low[q, pl.ds(at, planes), :] = low[rows]

    @pl.when((step >= zblocks) & (step < zblocks + quarters))
    def _():
        q = step - zblocks
        value = total[q] + (
            dot(high_ref[...], v_high[q])
            + (dot(low_ref[...], v_high[q]) + dot(high_ref[...], v_low[q]))
        )
        field[...] = value
        top = jnp.max(jnp.abs(value), axis=0, keepdims=True)
        for chunk in range(chunks):
            peaks[pl.ds(q * chunks + chunk, 1), :] = top[:, chunk * lanes : (chunk + 1) * lanes]
        slabs = col_ref.shape[1]
        for zblock in range(zblocks):
            for slab in range(slabs):
                target = (zblock // 2) * slabs + col_ref[zblock, slab]
                low_row = zblock * planes + 2 * slab
                for chunk in range(chunks):
                    at = 4 * chunk + 2 * (zblock % 2)
                    out_ref[target, at : at + 2, :] = field[
                        low_row : low_row + 2, chunk * lanes : (chunk + 1) * lanes
                    ]

    @pl.when(step == zblocks + quarters)
    def _():
        out_ref[...] = jnp.broadcast_to(peaks[...][None], out_ref.shape)


def middle(received, sizes, old_place, new_col, high, low):
    rows, cols, depth, lanes = received.shape
    zblocks = old_place.shape[0]
    height = high.shape[0]
    parts = rows * cols
    quarters = 4
    whole = pl.BlockSpec(high.shape, lambda i: (0, 0))
    smem = pl.BlockSpec(memory_space=pltpu.SMEM)
    return pl.pallas_call(
        middle_kernel,
        grid=(zblocks + quarters + 1,),
        in_specs=[
            smem,
            smem,
            smem,
            pl.BlockSpec(
                (rows, 1, depth, lanes), lambda i: (0, jnp.minimum(i, zblocks - 1), 0, 0)
            ),
            whole,
            whole,
        ],
        out_specs=pl.BlockSpec(
            (parts, 16, lanes), lambda i: (0, jnp.maximum(i - zblocks, 0), 0)
        ),
        out_shape=jax.ShapeDtypeStruct((parts, 16 * (quarters + 1), lanes), jnp.float32),
        scratch_shapes=[
            pltpu.VMEM((3, height + 40, lanes), jnp.float32),
            pltpu.VMEM((quarters, height, height), jnp.bfloat16),
            pltpu.VMEM((quarters, height, height), jnp.bfloat16),
            pltpu.VMEM((quarters, height, height), jnp.float32),
            pltpu.VMEM((height, height), jnp.float32),
            pltpu.VMEM((16, lanes), jnp.float32),
        ],
        compiler_params=pltpu.CompilerParams(vmem_limit_bytes=56 << 20),
        cost_estimate=pl.CostEstimate(
            flops=48 * height**3, bytes_accessed=20 << 20, transcendentals=0
        ),
        name="middle",
    )(sizes, old_place, new_col, received, high, low)


def finish_kernel(g_ref, p_ref, out_ref, peak_ref):
    parts, rows, lanes = g_ref.shape
    flat = g_ref.reshape(parts * rows, lanes)
    tops = p_ref.reshape(parts * rows, lanes)
    thick = out_ref.shape[0]
    chunks = rows // thick
    q = pl.program_id(0)
    for chunk in range(chunks):
        ys = slice(chunk * lanes, (chunk + 1) * lanes)
        for plane in range(thick):
            out_ref[plane, ys, :] = flat[pl.ds(chunk * thick + plane, parts, stride=rows), :].T
        peak_ref[ys, :] = tops[pl.ds(q * chunks + chunk, parts, stride=rows), :].T


def finish(received, thick, height):
    parts, rows, lanes = received.shape
    quarters = rows // 16 - 1
    return pl.pallas_call(
        finish_kernel,
        grid=(quarters,),
        in_specs=[
            pl.BlockSpec((parts, 16, lanes), lambda q: (0, q, 0)),
            pl.BlockSpec((parts, 16, lanes), lambda q: (0, quarters, 0)),
        ],
        out_specs=[
            pl.BlockSpec((thick, height, parts), lambda q: (0, 0, q)),
            pl.BlockSpec((height, parts), lambda q: (0, q)),
        ],
        out_shape=[
            jax.ShapeDtypeStruct((thick, height, quarters * parts), jnp.float32),
            jax.ShapeDtypeStruct((height, quarters * parts), jnp.float32),
        ],
        compiler_params=pltpu.CompilerParams(vmem_limit_bytes=48 << 20),
        cost_estimate=pl.CostEstimate(flops=1 << 20, bytes_accessed=10 << 20, transcendentals=0),
        name="finish",
    )(received, received)


def exchange(blocks):
    return lax.all_to_all(blocks, BOTH, split_axis=0, concat_axis=0, tiled=True)


def on_device(velocity, y_sizes, old_place, new_col):
    fields, _, places, depth, planes, width = velocity.shape
    rows, cols = lax.axis_size("row"), lax.axis_size("col")
    parts = rows * cols
    matrix = spectral_matrix(width)
    high, low = two_halves(matrix)
    high_t, low_t = two_halves(matrix.T)
    arrived = spread(
        velocity.reshape(fields, places * depth, planes, width), high_t, low_t, parts
    ).reshape(rows, cols, fields * places * depth, parts)
    shares = middle(arrived, y_sizes, old_place, new_col, high, low)
    field, peak = finish(exchange(shares), 4, width)
    return field.reshape(2, 1, 2, width, width), peak


def solution(mesh):
    in_specs = (P(None, "col", "row", None, None, None), P(), P(), P())
    out_specs = (P("row", "col", None, None, None), P())
    return jax.shard_map(
        on_device, mesh=mesh, in_specs=in_specs, out_specs=out_specs, check_vma=False
    )
```

```python
import math

import jax
import jax.numpy as jnp
import numpy as np
from jax import lax
from jax.experimental import pallas as pl
from jax.experimental.pallas import tpu as pltpu
from jax.sharding import PartitionSpec as P


def spectral_matrix(count):
    gap = (np.arange(count)[:, None] - np.arange(count)[None, :]) % count
    angle = gap.astype(np.float64) * (math.pi / count)
    parity = 1.0 - 2.0 * (gap % 2)
    divisor = np.where(gap == 0, 1.0, np.sin(angle))
    return np.where(gap == 0, 0.0, parity * np.cos(angle) / divisor * (2.0 / count))


def two_halves(matrix):
    high = matrix.astype(np.float32).astype(jnp.bfloat16)
    low = (matrix - high.astype(np.float64)).astype(np.float32).astype(jnp.bfloat16)
    return jnp.asarray(high), jnp.asarray(low)


def split(value):
    high = value.astype(jnp.bfloat16)
    return high, (value - high.astype(jnp.float32)).astype(jnp.bfloat16)


def dot(a, b):
    return jnp.dot(a, b, preferred_element_type=jnp.float32)


def fused_kernel(
    v_ref, high_ref, low_ref, sizes_ref, place_ref, col_ref, out_ref,
    stage, send, in_z, in_y, in_x, aligned, v_high, v_low, total, field, shares, peaks,
    ends, bounds, source, slab_of,
    in_sems, send_sem, recv_sems, share_send_sem, share_recv_sems, own_sem,
):
    fields, rows, planes, width = v_ref.shape
    lanes = send.shape[2]
    parts = lanes
    chunk = send.shape[1] // parts
    per_field = rows // 8
    groups = fields * per_field
    per_chunk = chunk // 8
    chunks_per_field = rows // chunk
    slots = stage.shape[0]
    quarters = total.shape[0]
    height = total.shape[2]
    pieces = height // lanes
    zblocks, blocks = place_ref.shape
    depth = rows // 2
    pad = (in_z.shape[0] - parts * rows) // 2
    arrivals = (in_z, in_y, in_x)
    row, col = lax.axis_index("row"), lax.axis_index("col")
    me = row * 16 + col
    x, y, z, core = (row // 4) * 2 + (col // 2) % 2, row % 4, col // 4, col % 2

    def load(n):
        return pltpu.make_async_copy(
            v_ref.at[fields - 1 - n // per_field, pl.ds((n % per_field) * 8, 8)],
            stage.at[n % slots],
            in_sems.at[n % slots],
        )

    def to_all(copy):
        def one(i, _):
            offset = ((i + core * (parts - 2 * i)) * 37) % parts
            there_x = (x + offset // 32) % 4
            there_y = (y + (offset // 8) % 4) % 4
            there_z = (z + (offset // 2) % 4) % 4
            there_core = (core + offset % 2) % 2
            to_row = (there_x // 2) * 4 + there_y
            to_col = there_z * 4 + (there_x % 2) * 2 + there_core
            src, dst, sent, got = copy(to_row * 16 + to_col)
            pltpu.make_async_remote_copy(
                src_ref=src,
                dst_ref=dst,
                send_sem=sent,
                recv_sem=got,
                device_id=(to_row, to_col),
                device_id_type=pl.DeviceIdType.MESH,
            ).start()
            return 0

        lax.fori_loop(1, parts, one, 0)

    def post(j, f):
        arrival = arrivals[f]
        at = pl.ds(pl.multiple_of(pad + me * rows + (j - f * chunks_per_field) * chunk, 8), chunk)
        to_all(
            lambda part: (
                send.at[j, pl.ds(pl.multiple_of(part * chunk, 8), chunk)],
                arrival.at[at],
                send_sem,
                recv_sems.at[f],
            )
        )
        arrival[at, :] = send[j, pl.ds(pl.multiple_of(me * chunk, 8), chunk), :]

    def group(n, f, slope_of):
        load(n).wait()
        value = slope_of(stage.at[n % slots])
        for r in range(8):
            piece = value(r)
            stacked = jnp.concatenate(
                [piece[:, q * parts : (q + 1) * parts] for q in range(width // parts)], axis=0
            )
            at = pl.ds((n % per_chunk) * 8 + r, parts, stride=chunk)
            send[n // per_chunk, at, :] = stacked.T

        @pl.when(n + slots < groups)
        def _():
            load(n + slots).start()

        if f > 0:

            @pl.when(n == f * per_field)
            def _():
                post(f * chunks_per_field - 1, f - 1)

        @pl.when((n % per_chunk == 0) & (n > f * per_field))
        def _():
            post(n // per_chunk - 1, f)

        return 0

    def plain(ref):
        return lambda r: ref[r]

    def along_x(ref):
        high, low = split(ref[...].reshape(8 * planes, width))
        slope = dot(high, high_ref[...]) + (dot(high, low_ref[...]) + dot(low, high_ref[...]))
        return lambda r: -slope[r * planes : (r + 1) * planes]

    for n in range(slots):
        load(n).start()
    for f in range(fields):
        slope_of = along_x if f == fields - 1 else plain
        lax.fori_loop(
            f * per_field,
            (f + 1) * per_field,
            lambda n, _, f=f, slope_of=slope_of: group(n, f, slope_of),
            0,
        )
    post(groups // per_chunk - 1, fields - 1)

    end = 0
    for b in range(blocks):
        end = end + sizes_ref[b]
        ends[b] = end
    windows = height // 8

    def window(g, _):
        first = 0
        for b in range(blocks - 1):
            first = first + jnp.where(ends[b] <= 8 * g, 1, 0)
        block = [first, jnp.minimum(first + 1, blocks - 1), jnp.minimum(first + 2, blocks - 1)]
        bounds[2 * g] = ends[block[0]]
        bounds[2 * g + 1] = ends[block[1]]
        skip = [jnp.clip(8 * g - ends[b] + sizes_ref[b], -8, depth - 1) + pad for b in block]

        def on_zblock(c, _):
            for k in range(3):
                place = place_ref[c, block[k]]
                source[c * 3 * windows + 3 * g + k] = (
                    skip[k] + ((place // 2) * 16 + c) * rows + (place % 2) * depth
                )
            return 0

        lax.fori_loop(0, zblocks, on_zblock, 0)
        return 0

    lax.fori_loop(0, windows, window, 0)

    slabs = col_ref.shape[1]

    def holder(i, _):
        zblock, want = i // slabs, i % slabs
        slab = 0
        for h in range(1, slabs):
            slab = jnp.where(col_ref[zblock, h] == want, h, slab)
        slab_of[i] = zblock * planes + 2 * slab
        return 0

    lax.fori_loop(0, zblocks * slabs, holder, 0)

    def arrived(f):
        block = arrivals[f].at[pl.ds(pad, (parts - 1) * rows)]
        pltpu.make_async_copy(block, block, recv_sems.at[f]).wait()

    def align(buffer, c):
        for g in range(windows):
            base = c * 3 * windows + 3 * g
            at = lax.broadcasted_iota(jnp.int32, (8, lanes), 0) + 8 * g
            one, two, three = (buffer[pl.ds(source[base + k], 8), :] for k in range(3))
            value = jnp.where(
                at < bounds[2 * g], one, jnp.where(at < bounds[2 * g + 1], two, three)
            )
            aligned[8 * g : 8 * g + 8, :] = value

    def on_z(c, _):
        align(in_z, c)
        high, low = split(aligned[...].T)
        at = pl.ds(pl.multiple_of(c * planes, planes), planes)
        for q in range(quarters):
            v_high[q, at, :] = high[q * planes : (q + 1) * planes]
            v_low[q, at, :] = low[q * planes : (q + 1) * planes]
        return 0

    def on_y(c, _):
        align(in_y, c)
        high, low = split(aligned[...])
        slope = dot(high_ref[...], high) + (dot(low_ref[...], high) + dot(high_ref[...], low))
        slope = slope.T
        at = pl.ds(pl.multiple_of(c * planes, planes), planes)
        for q in range(quarters):
            total[q, at, :] = slope[q * planes : (q + 1) * planes]
        return 0

    def on_x(c, _):
        align(in_x, c)
        slope = aligned[...].T
        at = pl.ds(pl.multiple_of(c * planes, planes), planes)
        for q in range(quarters):
            total[q, at, :] = total[q, at, :] + slope[q * planes : (q + 1) * planes]
        return 0

    for f, work in enumerate((on_z, on_y, on_x)):
        arrived(f)
        lax.fori_loop(0, zblocks, work, 0)

    block_rows = shares.shape[1] // parts
    mine = pl.ds(pl.multiple_of(me * block_rows, 8), block_rows)

    def quarter(q, _):
        value = total[q] + (
            dot(high_ref[...], v_high[q])
            + (dot(low_ref[...], v_high[q]) + dot(high_ref[...], v_low[q]))
        )
        top = jnp.max(jnp.abs(value), axis=0, keepdims=True)
        for piece in range(pieces):
            along = slice(piece * lanes, (piece + 1) * lanes)
            field[piece * height : (piece + 1) * height, :] = value[:, along]
            peaks[pl.ds(q * pieces + piece, 1), :] = top[:, along]
        for zblock in range(zblocks):
            for holding in range(slabs):
                low_row = slab_of[zblock * slabs + holding]
                target = ((zblock // 2) * slabs + holding) * block_rows + 2 * (zblock % 2)
                for piece in range(pieces):
                    at = target + 4 * piece
                    shares[q, at : at + 2, :] = field[pl.ds(low_row + piece * height, 2), :]
        to_all(
            lambda part: (
                shares.at[q, pl.ds(pl.multiple_of(part * block_rows, 8), block_rows)],
                out_ref.at[q, mine],
                share_send_sem,
                share_recv_sems,
            )
        )
        pltpu.make_async_copy(shares.at[q, mine], out_ref.at[q, mine], own_sem).start()
        return 0

    lax.fori_loop(0, quarters, quarter, 0)
    to_all(lambda part: (peaks, out_ref.at[quarters, mine], share_send_sem, share_recv_sems))
    pltpu.make_async_copy(peaks, out_ref.at[quarters, mine], own_sem).start()

    others = out_ref.at[:, pl.ds(0, (parts - 1) * block_rows)]
    own = out_ref.at[:, pl.ds(0, block_rows)]
    sent = send.at[:, pl.ds(0, (parts - 1) * chunk)]
    pltpu.make_async_copy(sent, sent, send_sem).wait()
    pltpu.make_async_copy(own, own, own_sem).wait()
    pltpu.make_async_copy(others, others, share_send_sem).wait()
    pltpu.make_async_copy(others, others, share_recv_sems).wait()


def fused(velocity, high, low, sizes, old_place, new_col, parts):
    fields, rows, planes, width = velocity.shape
    lanes = planes * width // parts
    height = width
    chunk = 24
    quarters = width // parts
    zblocks, blocks = old_place.shape
    block_rows = 16
    vmem = pl.BlockSpec(memory_space=pltpu.VMEM)
    smem = pl.BlockSpec(memory_space=pltpu.SMEM)
    anywhere = pl.BlockSpec(memory_space=pl.ANY)
    arrival = pltpu.VMEM((parts * rows + 16, lanes), jnp.float32)
    return pl.pallas_call(
        fused_kernel,
        in_specs=[anywhere, vmem, vmem, smem, smem, smem],
        out_specs=anywhere,
        out_shape=jax.ShapeDtypeStruct((quarters + 1, parts * block_rows, lanes), jnp.float32),
        scratch_shapes=[
            pltpu.VMEM((3, 8, planes, width), jnp.float32),
            pltpu.VMEM((fields * rows // chunk, parts * chunk, lanes), jnp.float32),
            arrival,
            arrival,
            arrival,
            pltpu.VMEM((height, lanes), jnp.float32),
            pltpu.VMEM((quarters, height, height), jnp.bfloat16),
            pltpu.VMEM((quarters, height, height), jnp.bfloat16),
            pltpu.VMEM((quarters, height, height), jnp.float32),
            pltpu.VMEM((height * height // lanes, lanes), jnp.float32),
            pltpu.VMEM((quarters, parts * block_rows, lanes), jnp.float32),
            pltpu.VMEM((block_rows, lanes), jnp.float32),
            pltpu.SMEM((blocks,), jnp.int32),
            pltpu.SMEM((height // 4,), jnp.int32),
            pltpu.SMEM((zblocks * 3 * height // 8,), jnp.int32),
            pltpu.SMEM((zblocks * new_col.shape[1],), jnp.int32),
            pltpu.SemaphoreType.DMA((3,)),
            pltpu.SemaphoreType.DMA,
            pltpu.SemaphoreType.DMA((3,)),
            pltpu.SemaphoreType.DMA,
            pltpu.SemaphoreType.DMA,
            pltpu.SemaphoreType.DMA,
        ],
        compiler_params=pltpu.CompilerParams(vmem_limit_bytes=63 << 20, has_side_effects=True),
        cost_estimate=pl.CostEstimate(
            flops=54 * height**3, bytes_accessed=32 << 20, transcendentals=0
        ),
        name="fused",
    )(velocity, high, low, sizes, old_place, new_col)


def finish_kernel(g_ref, p_ref, out_ref, peak_ref):
    thick, _, parts = out_ref.shape
    rows, lanes = g_ref.shape[1] // parts, g_ref.shape[2]
    chunks = rows // thick
    q = pl.program_id(0)
    for chunk in range(chunks):
        ys = slice(chunk * lanes, (chunk + 1) * lanes)
        for plane in range(thick):
            at = pl.ds(chunk * thick + plane, parts, stride=rows)
            out_ref[plane, ys, :] = g_ref[0, at, :].T
        peak_ref[ys, :] = p_ref[0, pl.ds(q * chunks + chunk, parts, stride=rows), :].T


def finish(received, parts, thick, height):
    quarters = received.shape[0] - 1
    block = (1,) + received.shape[1:]
    return pl.pallas_call(
        finish_kernel,
        grid=(quarters,),
        in_specs=[
            pl.BlockSpec(block, lambda q: (q, 0, 0)),
            pl.BlockSpec(block, lambda q: (quarters, 0, 0)),
        ],
        out_specs=[
            pl.BlockSpec((thick, height, parts), lambda q: (0, 0, q)),
            pl.BlockSpec((height, parts), lambda q: (0, q)),
        ],
        out_shape=[
            jax.ShapeDtypeStruct((thick, height, quarters * parts), jnp.float32),
            jax.ShapeDtypeStruct((height, quarters * parts), jnp.float32),
        ],
        compiler_params=pltpu.CompilerParams(vmem_limit_bytes=48 << 20),
        cost_estimate=pl.CostEstimate(flops=1 << 20, bytes_accessed=10 << 20, transcendentals=0),
        name="finish",
    )(received, received)


def on_device(velocity, y_sizes, old_place, new_col):
    fields, _, places, depth, planes, width = velocity.shape
    parts = lax.axis_size("row") * lax.axis_size("col")
    high, low = two_halves(spectral_matrix(width))
    received = fused(
        velocity.reshape(fields, places * depth, planes, width),
        high,
        low,
        y_sizes,
        old_place,
        new_col,
        parts,
    )
    field, peak = finish(received, parts, 4, width)
    return field.reshape(2, 1, 2, width, width), peak


def solution(mesh):
    in_specs = (P(None, "col", "row", None, None, None), P(), P(), P())
    out_specs = (P("row", "col", None, None, None), P())
    return jax.shard_map(
        on_device, mesh=mesh, in_specs=in_specs, out_specs=out_specs, check_vma=False
    )
```

```python
import math

import jax
import jax.numpy as jnp
import numpy as np
from jax import lax
from jax.experimental import pallas as pl
from jax.experimental.pallas import tpu as pltpu
from jax.sharding import PartitionSpec as P


def spectral_matrix(count):
    gap = (np.arange(count)[:, None] - np.arange(count)[None, :]) % count
    angle = gap.astype(np.float64) * (math.pi / count)
    parity = 1.0 - 2.0 * (gap % 2)
    divisor = np.where(gap == 0, 1.0, np.sin(angle))
    return np.where(gap == 0, 0.0, parity * np.cos(angle) / divisor * (2.0 / count))


def two_halves(matrix):
    high = matrix.astype(np.float32).astype(jnp.bfloat16)
    low = (matrix - high.astype(np.float64)).astype(np.float32).astype(jnp.bfloat16)
    return jnp.asarray(high), jnp.asarray(low)


def split(value):
    high = value.astype(jnp.bfloat16)
    return high, (value - high.astype(jnp.float32)).astype(jnp.bfloat16)


def dot(a, b):
    return jnp.dot(a, b, preferred_element_type=jnp.float32)


def fused_kernel(
    v_ref, high_ref, low_ref, sizes_ref, place_ref, col_ref, out_ref,
    stage, send, in_x, in_a, in_b, aligned, z_high, z_low, y_high, y_low, total, field, shares,
    ends, bounds, source, slab_of,
    in_sems, send_sem, recv_sems, share_send_sems, share_recv_sems, own_sem,
):
    fields, rows, planes, width = v_ref.shape
    lanes = send.shape[2]
    parts = lanes
    chunk = send.shape[1] // parts
    per_field = rows // 8
    groups = fields * per_field
    per_chunk = chunk // 8
    chunks_per_field = rows // chunk
    slots = stage.shape[0]
    quarters = total.shape[0]
    half = quarters // 2
    height = total.shape[2]
    pieces = height // lanes
    zblocks, blocks = place_ref.shape
    slabs = col_ref.shape[1]
    depth = rows // 2
    pad = (in_x.shape[0] - parts * rows) // 2
    arrivals = (in_x, in_a, in_b)
    row, col = lax.axis_index("row"), lax.axis_index("col")
    me = row * 16 + col
    x, y, z, core = (row // 4) * 2 + (col // 2) % 2, row % 4, col // 4, col % 2

    def partner(i):
        offset = ((i + core * (parts - 2 * i)) * 37) % parts
        there_x = (x + offset // 32) % 4
        there_y = (y + (offset // 8) % 4) % 4
        there_z = (z + (offset // 2) % 4) % 4
        there_core = (core + offset % 2) % 2
        return (there_x // 2) * 4 + there_y, there_z * 4 + (there_x % 2) * 2 + there_core

    barrier = pltpu.get_barrier_semaphore()

    def greet(i, _):
        pl.semaphore_signal(
            barrier, inc=1, device_id=partner(i), device_id_type=pl.DeviceIdType.MESH
        )
        return 0

    def loads(f, n):
        at = pl.ds((n - f * per_field) * 8, 8)
        slot = n % slots
        if f == 0:
            return [pltpu.make_async_copy(v_ref.at[0, at], stage.at[slot], in_sems.at[slot, 0])]
        wide = width // 2
        xs = pl.ds((f - 1) * wide, wide)
        return [
            pltpu.make_async_copy(
                v_ref.at[2 - k, at, :, xs],
                stage.at[slot, :, :, pl.ds(k * wide, wide)],
                in_sems.at[slot, k],
            )
            for k in range(2)
        ]

    def start_load(f, n):
        for copy in loads(f, n):
            copy.start()

    def to_all(copy):
        def one(i, _):
            to_row, to_col = partner(i)
            src, dst, sent, got = copy(to_row * 16 + to_col)
            pltpu.make_async_remote_copy(
                src_ref=src,
                dst_ref=dst,
                send_sem=sent,
                recv_sem=got,
                device_id=(to_row, to_col),
                device_id_type=pl.DeviceIdType.MESH,
            ).start()
            return 0

        lax.fori_loop(1, parts, one, 0)

    def post(j, f):
        arrival = arrivals[f]
        at = pl.ds(pl.multiple_of(pad + me * rows + (j - f * chunks_per_field) * chunk, 8), chunk)
        to_all(
            lambda part: (
                send.at[j, pl.ds(pl.multiple_of(part * chunk, 8), chunk)],
                arrival.at[at],
                send_sem,
                recv_sems.at[f],
            )
        )
        arrival[at, :] = send[j, pl.ds(pl.multiple_of(me * chunk, 8), chunk), :]

    def group(n, f, slope_of):
        for copy in loads(f, n):
            copy.wait()
        value = slope_of(stage.at[n % slots])
        for r in range(8):
            piece = value(r)
            stacked = jnp.concatenate(
                [piece[:, q * parts : (q + 1) * parts] for q in range(width // parts)], axis=0
            )
            at = pl.ds((n % per_chunk) * 8 + r, parts, stride=chunk)
            send[n // per_chunk, at, :] = stacked.T

        later = n + slots
        for g in range(f, min(f + 2, fields)):

            @pl.when((later >= g * per_field) & (later < (g + 1) * per_field))
            def _(g=g):
                start_load(g, later)

        if f > 0:

            @pl.when(n == f * per_field)
            def _():
                post(f * chunks_per_field - 1, f - 1)

        @pl.when((n % per_chunk == 0) & (n > f * per_field))
        def _():
            post(n // per_chunk - 1, f)

        return 0

    def plain(ref):
        return lambda r: ref[r]

    def along_x(ref):
        high, low = split(ref[...].reshape(8 * planes, width))
        slope = dot(high, high_ref[...]) + (dot(high, low_ref[...]) + dot(low, high_ref[...]))
        return lambda r: -slope[r * planes : (r + 1) * planes]

    lax.fori_loop(1, parts, greet, 0)
    for n in range(slots):
        start_load(0, n)
    pl.semaphore_wait(barrier, parts - 1)
    for f in range(fields):
        slope_of = plain if f else along_x
        lax.fori_loop(
            f * per_field,
            (f + 1) * per_field,
            lambda n, _, f=f, slope_of=slope_of: group(n, f, slope_of),
            0,
        )
    post(groups // per_chunk - 1, fields - 1)

    end = 0
    for b in range(blocks):
        end = end + sizes_ref[b]
        ends[b] = end
    windows = height // 8

    def window(g, _):
        first = 0
        for b in range(blocks - 1):
            first = first + jnp.where(ends[b] <= 8 * g, 1, 0)
        block = [first, jnp.minimum(first + 1, blocks - 1), jnp.minimum(first + 2, blocks - 1)]
        bounds[2 * g] = ends[block[0]]
        bounds[2 * g + 1] = ends[block[1]]
        skip = [jnp.clip(8 * g - ends[b] + sizes_ref[b], -8, depth - 1) + pad for b in block]

        def on_zblock(c, _):
            for k in range(3):
                place = place_ref[c, block[k]]
                source[c * 3 * windows + 3 * g + k] = (
                    skip[k] + ((place >> 1) * 16 + c) * rows + (place & 1) * depth
                )
            return 0

        lax.fori_loop(0, zblocks, on_zblock, 0)
        return 0

    lax.fori_loop(0, windows, window, 0)

    def holder(i, _):
        zblock, want = i // slabs, i % slabs
        slab = 0
        for h in range(1, slabs):
            slab = jnp.where(col_ref[zblock, h] == want, h, slab)
        slab_of[i] = zblock * planes + 2 * slab
        return 0

    lax.fori_loop(0, zblocks * slabs, holder, 0)

    def arrived(f):
        block = arrivals[f].at[pl.ds(pad, (parts - 1) * rows)]
        pltpu.make_async_copy(block, block, recv_sems.at[f]).wait()

    def align(buffer, c):
        for g in range(windows):
            base = c * 3 * windows + 3 * g
            at = lax.broadcasted_iota(jnp.int32, (8, lanes), 0) + 8 * g
            one, two, three = (buffer[pl.ds(source[base + k], 8), :] for k in range(3))
            value = jnp.where(
                at < bounds[2 * g], one, jnp.where(at < bounds[2 * g + 1], two, three)
            )
            aligned[8 * g : 8 * g + 8, :] = value

    def on_x(c, _):
        align(in_x, c)
        slope = aligned[...].T
        at = pl.ds(pl.multiple_of(c * planes, planes), planes)
        for q in range(quarters):
            total[q, at, :] = slope[q * planes : (q + 1) * planes]
        return 0

    def on_half(h, c):
        align(arrivals[1 + h], c)
        high, low = split(aligned[...].T)
        at = pl.ds(pl.multiple_of(c * planes, planes), planes)
        for q in range(half):
            zs = slice(q * planes, (q + 1) * planes)
            ys = slice((half + q) * planes, (half + q + 1) * planes)
            z_high[half * h + q, at, :] = high[zs]
            z_low[half * h + q, at, :] = low[zs]
            y_high[half * h + q, at, :] = high[ys]
            y_low[half * h + q, at, :] = low[ys]
        return 0

    block_rows = shares.shape[1] // parts
    mine = pl.ds(pl.multiple_of(me * block_rows, 8), block_rows)

    def quarter(h, k):
        q = half * h + k
        along_z = dot(high_ref[...], z_high[q]) + (
            dot(low_ref[...], z_high[q]) + dot(high_ref[...], z_low[q])
        )
        along_y = dot(y_high[q], high_ref[...]) + (
            dot(y_high[q], low_ref[...]) + dot(y_low[q], high_ref[...])
        )
        value = total[q] + (along_z - along_y)
        top = jnp.max(jnp.abs(value), axis=0, keepdims=True)
        for piece in range(pieces):
            along = slice(piece * lanes, (piece + 1) * lanes)
            field[piece * height : (piece + 1) * height, :] = value[:, along]
            aligned[pl.ds(k * pieces + piece, 1), :] = top[:, along]
        first = pl.multiple_of(k * 4 * pieces, 8)
        for zblock in range(zblocks):
            for holding in range(slabs):
                low_row = slab_of[zblock * slabs + holding]
                target = ((zblock // 2) * slabs + holding) * block_rows + 2 * (zblock % 2)
                for piece in range(pieces):
                    shares[h, pl.ds(first + target + 4 * piece, 2), :] = field[
                        pl.ds(low_row + piece * height, 2), :
                    ]
        return 0

    arrived(0)
    lax.fori_loop(0, zblocks, on_x, 0)
    for h in range(2):
        arrived(1 + h)
        lax.fori_loop(0, zblocks, lambda c, _, h=h: on_half(h, c), 0)
        lax.fori_loop(0, half, lambda k, _, h=h: quarter(h, k), 0)
        tops = aligned[: half * pieces, :]

        def top_rows(part, _, h=h, tops=tops):
            at = pl.multiple_of(part * block_rows + half * 4 * pieces, 8)
            shares[h, pl.ds(at, half * pieces), :] = tops
            return 0

        lax.fori_loop(0, parts, top_rows, 0)
        to_all(
            lambda part, h=h: (
                shares.at[h, pl.ds(pl.multiple_of(part * block_rows, 8), block_rows)],
                out_ref.at[h, mine],
                share_send_sems.at[h],
                share_recv_sems.at[h],
            )
        )
        pltpu.make_async_copy(shares.at[h, mine], out_ref.at[h, mine], own_sem.at[h]).start()

    sent = send.at[:, pl.ds(0, (parts - 1) * chunk)]
    pltpu.make_async_copy(sent, sent, send_sem).wait()
    for h in range(2):
        others = out_ref.at[h, pl.ds(0, (parts - 1) * block_rows)]
        own = out_ref.at[h, pl.ds(0, block_rows)]
        pltpu.make_async_copy(own, own, own_sem.at[h]).wait()
        pltpu.make_async_copy(others, others, share_send_sems.at[h]).wait()
        pltpu.make_async_copy(others, others, share_recv_sems.at[h]).wait()


def fused(velocity, high, low, sizes, old_place, new_col, parts):
    fields, rows, planes, width = velocity.shape
    lanes = planes * width // parts
    height = width
    chunk = 24
    quarters = width // parts
    zblocks, blocks = old_place.shape
    block_rows = 40
    vmem = pl.BlockSpec(memory_space=pltpu.VMEM)
    smem = pl.BlockSpec(memory_space=pltpu.SMEM)
    anywhere = pl.BlockSpec(memory_space=pl.ANY)
    arrival = pltpu.VMEM((parts * rows + 16, lanes), jnp.float32)
    operand = pltpu.VMEM((quarters, height, height), jnp.bfloat16)
    return pl.pallas_call(
        fused_kernel,
        in_specs=[anywhere, vmem, vmem, smem, smem, smem],
        out_specs=anywhere,
        out_shape=jax.ShapeDtypeStruct((2, parts * block_rows, lanes), jnp.float32),
        scratch_shapes=[
            pltpu.VMEM((3, 8, planes, width), jnp.float32),
            pltpu.VMEM((fields * rows // chunk, parts * chunk, lanes), jnp.float32),
            arrival,
            arrival,
            arrival,
            pltpu.VMEM((height, lanes), jnp.float32),
            operand,
            operand,
            operand,
            operand,
            pltpu.VMEM((quarters, height, height), jnp.float32),
            pltpu.VMEM((height * height // lanes, lanes), jnp.float32),
            pltpu.VMEM((2, parts * block_rows, lanes), jnp.float32),
            pltpu.SMEM((blocks,), jnp.int32),
            pltpu.SMEM((height // 4,), jnp.int32),
            pltpu.SMEM((zblocks * 3 * height // 8,), jnp.int32),
            pltpu.SMEM((zblocks * new_col.shape[1],), jnp.int32),
            pltpu.SemaphoreType.DMA((3, 2)),
            pltpu.SemaphoreType.DMA,
            pltpu.SemaphoreType.DMA((3,)),
            pltpu.SemaphoreType.DMA((2,)),
            pltpu.SemaphoreType.DMA((2,)),
            pltpu.SemaphoreType.DMA((2,)),
        ],
        compiler_params=pltpu.CompilerParams(
            vmem_limit_bytes=63 << 20, has_side_effects=True, collective_id=0
        ),
        cost_estimate=pl.CostEstimate(
            flops=54 * height**3, bytes_accessed=32 << 20, transcendentals=0
        ),
        name="fused",
    )(velocity, high, low, sizes, old_place, new_col)


def finish_kernel(g_ref, out_ref, peak_ref):
    thick, height, parts = out_ref.shape
    rows, lanes = g_ref.shape[1] // parts, g_ref.shape[2]
    chunks = height // lanes
    k = pl.program_id(0) % 2
    for chunk in range(chunks):
        ys = slice(chunk * lanes, (chunk + 1) * lanes)
        for plane in range(thick):
            at = pl.ds((k * chunks + chunk) * thick + plane, parts, stride=rows)
            out_ref[plane, ys, :] = g_ref[0, at, :].T
        tops = pl.ds(2 * chunks * thick + k * chunks + chunk, parts, stride=rows)
        peak_ref[ys, :] = g_ref[0, tops, :].T


def finish(received, parts, thick, height):
    quarters = height // parts
    return pl.pallas_call(
        finish_kernel,
        grid=(quarters,),
        in_specs=[pl.BlockSpec((1,) + received.shape[1:], lambda q: (q // 2, 0, 0))],
        out_specs=[
            pl.BlockSpec((thick, height, parts), lambda q: (0, 0, q)),
            pl.BlockSpec((height, parts), lambda q: (0, q)),
        ],
        out_shape=[
            jax.ShapeDtypeStruct((thick, height, quarters * parts), jnp.float32),
            jax.ShapeDtypeStruct((height, quarters * parts), jnp.float32),
        ],
        compiler_params=pltpu.CompilerParams(vmem_limit_bytes=63 << 20),
        cost_estimate=pl.CostEstimate(flops=1 << 20, bytes_accessed=10 << 20, transcendentals=0),
        name="finish",
    )(received)


def on_device(velocity, y_sizes, old_place, new_col):
    fields, _, places, depth, planes, width = velocity.shape
    parts = lax.axis_size("row") * lax.axis_size("col")
    high, low = two_halves(spectral_matrix(width))
    received = fused(
        velocity.reshape(fields, places * depth, planes, width),
        high,
        low,
        y_sizes,
        old_place,
        new_col,
        parts,
    )
    field, peak = finish(received, parts, 4, width)
    return field.reshape(2, 1, 2, width, width), peak


def solution(mesh):
    in_specs = (P(None, "col", "row", None, None, None), P(), P(), P())
    out_specs = (P("row", "col", None, None, None), P())
    return jax.shard_map(
        on_device, mesh=mesh, in_specs=in_specs, out_specs=out_specs, check_vma=False
    )
```

```python
import math

import jax
import jax.numpy as jnp
import numpy as np
from jax import lax
from jax.experimental import pallas as pl
from jax.experimental.pallas import tpu as pltpu
from jax.sharding import PartitionSpec as P


def spectral_matrix(count):
    gap = (np.arange(count)[:, None] - np.arange(count)[None, :]) % count
    angle = gap.astype(np.float64) * (math.pi / count)
    parity = 1.0 - 2.0 * (gap % 2)
    divisor = np.where(gap == 0, 1.0, np.sin(angle))
    return np.where(gap == 0, 0.0, parity * np.cos(angle) / divisor * (2.0 / count))


def two_halves(matrix):
    high = matrix.astype(np.float32).astype(jnp.bfloat16)
    low = (matrix - high.astype(np.float64)).astype(np.float32).astype(jnp.bfloat16)
    return jnp.asarray(high), jnp.asarray(low)


def split(value):
    high = value.astype(jnp.bfloat16)
    return high, (value - high.astype(jnp.float32)).astype(jnp.bfloat16)


def dot(a, b):
    return jnp.dot(a, b, preferred_element_type=jnp.float32)


def fused_kernel(
    v_ref, high_ref, low_ref, sizes_ref, place_ref, col_ref, out_ref, peak_ref,
    stage, send, in_a, in_x, in_b, aligned, z_high, z_low, y_high, y_low, total, field, shares,
    tops,
    ends, bounds, source, slab_of,
    in_sems, send_sem, recv_sems, share_send_sems, share_recv_sems, own_sem,
    peak_send_sems, peak_recv_sems, peak_own_sems, pair_send_sems, pair_recv_sems,
):
    fields, rows, planes, width = v_ref.shape
    lanes = send.shape[2]
    parts = lanes
    chunk = send.shape[1] // parts
    per_field = rows // 8
    groups = fields * per_field
    per_chunk = chunk // 8
    chunks_per_field = rows // chunk
    slots = stage.shape[0]
    quarters = total.shape[0]
    half = quarters // 2
    height = total.shape[2]
    pieces = height // lanes
    zblocks, blocks = place_ref.shape
    slabs = col_ref.shape[1]
    depth = rows // 2
    pad = (in_x.shape[0] - parts * rows) // 2
    arrivals = (in_a, in_x, in_b)
    x_section = 1
    row, col = lax.axis_index("row"), lax.axis_index("col")
    me = row * 16 + col
    div, rem = lax.div, lax.rem
    chip, core = row * 8 + div(col, 2), rem(col, 2)
    x, y = div(row, 4) * 2 + rem(div(col, 2), 2), rem(row, 4)
    z = div(col, 4)

    def chip_at(offset):
        there_x = rem(x + div(offset, 16), 4)
        there_y = rem(y + div(offset, 4), 4)
        there_z = rem(z + offset, 4)
        return div(there_x, 2) * 4 + there_y, there_z * 4 + rem(there_x, 2) * 2

    def partner(i):
        offset = rem((i + core * (parts - 2 * i)) * 37, parts)
        to_row, first = chip_at(div(offset, 2))
        return to_row, first + rem(core + offset, 2)

    barrier = pltpu.get_barrier_semaphore()

    def greet(i, _):
        other = rem(me + i, parts)
        pl.semaphore_signal(
            barrier,
            inc=1,
            device_id=(div(other, 16), rem(other, 16)),
            device_id_type=pl.DeviceIdType.MESH,
        )
        return 0

    def loads(f, n):
        at = pl.ds((n - f * per_field) * 8, 8)
        slot = n % slots
        if f == x_section:
            return [pltpu.make_async_copy(v_ref.at[0, at], stage.at[slot], in_sems.at[slot, 0])]
        wide = width // 2
        xs = pl.ds((f // 2) * wide, wide)
        return [
            pltpu.make_async_copy(
                v_ref.at[2 - k, at, :, xs],
                stage.at[slot, :, :, pl.ds(k * wide, wide)],
                in_sems.at[slot, k],
            )
            for k in range(2)
        ]

    def start_load(f, n):
        for copy in loads(f, n):
            copy.start()

    def to_all(copy):
        def one(i, _):
            to_row, to_col = partner(i)
            src, dst, sent, got = copy(to_row * 16 + to_col)
            pltpu.make_async_remote_copy(
                src_ref=src,
                dst_ref=dst,
                send_sem=sent,
                recv_sem=got,
                device_id=(to_row, to_col),
                device_id_type=pl.DeviceIdType.MESH,
            ).start()
            return 0

        lax.fori_loop(1, parts, one, 0)

    def post(j, f):
        arrival = arrivals[f]
        at = pl.ds(pl.multiple_of(pad + me * rows + (j - f * chunks_per_field) * chunk, 8), chunk)
        to_all(
            lambda part: (
                send.at[j, pl.ds(pl.multiple_of(part * chunk, 8), chunk)],
                arrival.at[at],
                send_sem,
                recv_sems.at[f],
            )
        )
        arrival[at, :] = send[j, pl.ds(pl.multiple_of(me * chunk, 8), chunk), :]

    def group(n, f, slope_of):
        for copy in loads(f, n):
            copy.wait()
        value = slope_of(stage.at[n % slots])
        for r in range(8):
            piece = value(r)
            stacked = jnp.concatenate(
                [piece[:, q * parts : (q + 1) * parts] for q in range(width // parts)], axis=0
            )
            at = pl.ds((n % per_chunk) * 8 + r, parts, stride=chunk)
            send[n // per_chunk, at, :] = stacked.T

        later = n + slots
        for g in range(f, min(f + 2, fields)):

            @pl.when((later >= g * per_field) & (later < (g + 1) * per_field))
            def _(g=g):
                start_load(g, later)

        if f > 0:

            @pl.when(n == f * per_field)
            def _():
                post(f * chunks_per_field - 1, f - 1)

        @pl.when((n % per_chunk == 0) & (n > f * per_field))
        def _():
            post(n // per_chunk - 1, f)

        return 0

    def plain(ref):
        return lambda r: ref[r]

    def along_x(ref):
        high, low = split(ref[...].reshape(8 * planes, width))
        slope = dot(high, high_ref[...]) + (dot(high, low_ref[...]) + dot(low, high_ref[...]))
        return lambda r: -slope[r * planes : (r + 1) * planes]

    lax.fori_loop(1, parts, greet, 0)
    for n in range(slots):
        start_load(0, n)
    pl.semaphore_wait(barrier, parts - 1)
    for f in range(fields):
        slope_of = along_x if f == x_section else plain
        lax.fori_loop(
            f * per_field,
            (f + 1) * per_field,
            lambda n, _, f=f, slope_of=slope_of: group(n, f, slope_of),
            0,
        )
    post(groups // per_chunk - 1, fields - 1)

    end = 0
    for b in range(blocks):
        end = end + sizes_ref[b]
        ends[b] = end
    windows = height // 8

    def window(g, _):
        first = 0
        for b in range(blocks - 1):
            first = first + jnp.where(ends[b] <= 8 * g, 1, 0)
        block = [first, jnp.minimum(first + 1, blocks - 1), jnp.minimum(first + 2, blocks - 1)]
        bounds[2 * g] = ends[block[0]]
        bounds[2 * g + 1] = ends[block[1]]
        skip = [jnp.clip(8 * g - ends[b] + sizes_ref[b], -8, depth - 1) + pad for b in block]

        def on_zblock(c, _):
            for k in range(3):
                place = place_ref[c, block[k]]
                source[c * 3 * windows + 3 * g + k] = (
                    skip[k] + ((place >> 1) * 16 + c) * rows + (place & 1) * depth
                )
            return 0

        lax.fori_loop(0, zblocks, on_zblock, 0)
        return 0

    lax.fori_loop(0, windows, window, 0)

    def holder(i, _):
        zblock, want = i // slabs, i % slabs
        slab = 0
        for h in range(1, slabs):
            slab = jnp.where(col_ref[zblock, h] == want, h, slab)
        slab_of[i] = zblock * planes + 2 * slab
        return 0

    lax.fori_loop(0, zblocks * slabs, holder, 0)

    def arrived(f):
        block = arrivals[f].at[pl.ds(pad, (parts - 1) * rows)]
        pltpu.make_async_copy(block, block, recv_sems.at[f]).wait()

    def align(buffer, c):
        for g in range(windows):
            base = c * 3 * windows + 3 * g
            at = lax.broadcasted_iota(jnp.int32, (8, lanes), 0) + 8 * g
            one, two, three = (buffer[pl.ds(source[base + k], 8), :] for k in range(3))
            value = jnp.where(
                at < bounds[2 * g], one, jnp.where(at < bounds[2 * g + 1], two, three)
            )
            aligned[8 * g : 8 * g + 8, :] = value

    def on_x(c, _):
        align(in_x, c)
        slope = aligned[...].T
        at = pl.ds(pl.multiple_of(c * planes, planes), planes)
        for q in range(quarters):
            total[q, at, :] = slope[q * planes : (q + 1) * planes]
        return 0

    def on_half(h, c):
        align(arrivals[2 * h], c)
        high, low = split(aligned[...].T)
        at = pl.ds(pl.multiple_of(c * planes, planes), planes)
        for q in range(half):
            zs = slice(q * planes, (q + 1) * planes)
            ys = slice((half + q) * planes, (half + q + 1) * planes)
            z_high[half * h + q, at, :] = high[zs]
            z_low[half * h + q, at, :] = low[zs]
            y_high[half * h + q, at, :] = high[ys]
            y_low[half * h + q, at, :] = low[ys]
        return 0

    block_rows = shares.shape[1] // parts
    mine = pl.ds(pl.multiple_of(me * block_rows, 8), block_rows)

    def quarter(h, k):
        q = half * h + k
        along_z = dot(high_ref[...], z_high[q]) + (
            dot(low_ref[...], z_high[q]) + dot(high_ref[...], z_low[q])
        )
        along_y = dot(y_high[q], high_ref[...]) + (
            dot(y_high[q], low_ref[...]) + dot(y_low[q], high_ref[...])
        )
        value = total[q] + (along_z - along_y)
        top = jnp.max(jnp.abs(value), axis=0, keepdims=True)
        for piece in range(pieces):
            along = slice(piece * lanes, (piece + 1) * lanes)
            field[piece * height : (piece + 1) * height, :] = value[:, along]
            tops[h, pl.ds(k * pieces + piece, 1), :] = top[:, along]
        first = pl.multiple_of(k * 4 * pieces, 8)
        for zblock in range(zblocks):
            for holding in range(slabs):
                low_row = slab_of[zblock * slabs + holding]
                target = ((zblock // 2) * slabs + holding) * block_rows + 2 * (zblock % 2)
                for piece in range(pieces):
                    shares[h, pl.ds(first + target + 4 * piece, 2), :] = field[
                        pl.ds(low_row + piece * height, 2), :
                    ]
        return 0

    def give_peaks(h):
        mine = peak_ref.at[h, chip, core]

        def one(i, _):
            to_row, first = chip_at(rem(i * 37, parts // 2))
            pltpu.make_async_remote_copy(
                src_ref=tops.at[h],
                dst_ref=mine,
                send_sem=peak_send_sems.at[h],
                recv_sem=peak_recv_sems.at[h],
                device_id=(to_row, first + core),
                device_id_type=pl.DeviceIdType.MESH,
            ).start()
            return 0

        lax.fori_loop(1, parts // 2, one, 0)
        pltpu.make_async_copy(tops.at[h], mine, peak_own_sems.at[h]).start()

    def pair_copy(h):
        held = peak_ref.at[h, :, core]
        return pltpu.make_async_remote_copy(
            src_ref=held,
            dst_ref=held,
            send_sem=pair_send_sems.at[h],
            recv_sem=pair_recv_sems.at[h],
            device_id=(row, col + 1 - 2 * core),
            device_id_type=pl.DeviceIdType.MESH,
        )

    for h in range(2):
        arrived(2 * h)
        lax.fori_loop(0, zblocks, lambda c, _, h=h: on_half(h, c), 0)
        if h == 0:
            arrived(x_section)
            lax.fori_loop(0, zblocks, on_x, 0)
        lax.fori_loop(0, half, lambda k, _, h=h: quarter(h, k), 0)
        give_peaks(h)
        to_all(
            lambda part, h=h: (
                shares.at[h, pl.ds(pl.multiple_of(part * block_rows, 8), block_rows)],
                out_ref.at[h, mine],
                share_send_sems.at[h],
                share_recv_sems.at[h],
            )
        )
        pltpu.make_async_copy(shares.at[h, mine], out_ref.at[h, mine], own_sem.at[h]).start()

    for h in range(2):
        others = peak_ref.at[h, pl.ds(0, parts // 2 - 1), 0]
        pltpu.make_async_copy(tops.at[h], peak_ref.at[h, chip, core], peak_own_sems.at[h]).wait()
        pltpu.make_async_copy(others, others, peak_send_sems.at[h]).wait()
        pltpu.make_async_copy(others, others, peak_recv_sems.at[h]).wait()
        pair_copy(h).start()
    sent = send.at[:, pl.ds(0, (parts - 1) * chunk)]
    pltpu.make_async_copy(sent, sent, send_sem).wait()
    for h in range(2):
        pair_copy(h).wait()
        others = out_ref.at[h, pl.ds(0, (parts - 1) * block_rows)]
        own = out_ref.at[h, pl.ds(0, block_rows)]
        pltpu.make_async_copy(own, own, own_sem.at[h]).wait()
        pltpu.make_async_copy(others, others, share_send_sems.at[h]).wait()
        pltpu.make_async_copy(others, others, share_recv_sems.at[h]).wait()


def fused(velocity, high, low, sizes, old_place, new_col, parts):
    fields, rows, planes, width = velocity.shape
    lanes = planes * width // parts
    height = width
    chunk = 24
    quarters = width // parts
    zblocks, blocks = old_place.shape
    block_rows = 32
    vmem = pl.BlockSpec(memory_space=pltpu.VMEM)
    smem = pl.BlockSpec(memory_space=pltpu.SMEM)
    anywhere = pl.BlockSpec(memory_space=pl.ANY)
    arrival = pltpu.VMEM((parts * rows + 16, lanes), jnp.float32)
    operand = pltpu.VMEM((quarters, height, height), jnp.bfloat16)
    return pl.pallas_call(
        fused_kernel,
        in_specs=[anywhere, vmem, vmem, smem, smem, smem],
        out_specs=[anywhere, anywhere],
        out_shape=[
            jax.ShapeDtypeStruct((2, parts * block_rows, lanes), jnp.float32),
            jax.ShapeDtypeStruct((2, parts // 2, 2, 8, lanes), jnp.float32),
        ],
        scratch_shapes=[
            pltpu.VMEM((3, 8, planes, width), jnp.float32),
            pltpu.VMEM((fields * rows // chunk, parts * chunk, lanes), jnp.float32),
            arrival,
            arrival,
            arrival,
            pltpu.VMEM((height, lanes), jnp.float32),
            operand,
            operand,
            operand,
            operand,
            pltpu.VMEM((quarters, height, height), jnp.float32),
            pltpu.VMEM((height * height // lanes, lanes), jnp.float32),
            pltpu.VMEM((2, parts * block_rows, lanes), jnp.float32),
            pltpu.VMEM((2, 8, lanes), jnp.float32),
            pltpu.SMEM((blocks,), jnp.int32),
            pltpu.SMEM((height // 4,), jnp.int32),
            pltpu.SMEM((zblocks * 3 * height // 8,), jnp.int32),
            pltpu.SMEM((zblocks * new_col.shape[1],), jnp.int32),
            pltpu.SemaphoreType.DMA((3, 2)),
            pltpu.SemaphoreType.DMA,
            pltpu.SemaphoreType.DMA((3,)),
        ]
        + [pltpu.SemaphoreType.DMA((2,))] * 8,
        compiler_params=pltpu.CompilerParams(
            vmem_limit_bytes=63 << 20, has_side_effects=True, collective_id=0
        ),
        cost_estimate=pl.CostEstimate(
            flops=54 * height**3, bytes_accessed=32 << 20, transcendentals=0
        ),
        name="fused",
    )(velocity, high, low, sizes, old_place, new_col)


def finish_kernel(g_ref, p_ref, out_ref, peak_ref):
    thick, height, parts = out_ref.shape
    rows, lanes = g_ref.shape[1] // parts, g_ref.shape[2]
    chunks = height // lanes
    k = pl.program_id(0) % 2
    for chunk in range(chunks):
        ys = slice(chunk * lanes, (chunk + 1) * lanes)
        for plane in range(thick):
            at = pl.ds((k * chunks + chunk) * thick + plane, parts, stride=rows)
            out_ref[plane, ys, :] = g_ref[0, at, :].T
        tops = pl.ds(k * chunks + chunk, parts, stride=2 * chunks)
        peak_ref[ys, :] = p_ref[0, tops, :].T


def finish(received, tops, parts, thick, height):
    quarters = height // parts
    return pl.pallas_call(
        finish_kernel,
        grid=(quarters,),
        in_specs=[
            pl.BlockSpec((1,) + received.shape[1:], lambda q: (q // 2, 0, 0)),
            pl.BlockSpec((1,) + tops.shape[1:], lambda q: (q // 2, 0, 0)),
        ],
        out_specs=[
            pl.BlockSpec((thick, height, parts), lambda q: (0, 0, q)),
            pl.BlockSpec((height, parts), lambda q: (0, q)),
        ],
        out_shape=[
            jax.ShapeDtypeStruct((thick, height, quarters * parts), jnp.float32),
            jax.ShapeDtypeStruct((height, quarters * parts), jnp.float32),
        ],
        compiler_params=pltpu.CompilerParams(vmem_limit_bytes=32 << 20),
        cost_estimate=pl.CostEstimate(flops=1 << 20, bytes_accessed=10 << 20, transcendentals=0),
        name="finish",
    )(received, tops)


def on_device(velocity, y_sizes, old_place, new_col):
    fields, _, places, depth, planes, width = velocity.shape
    parts = lax.axis_size("row") * lax.axis_size("col")
    high, low = two_halves(spectral_matrix(width))
    received, tops = fused(
        velocity.reshape(fields, places * depth, planes, width),
        high,
        low,
        y_sizes,
        old_place,
        new_col,
        parts,
    )
    tops = tops.reshape(2, parts * 8, parts)
    field, peak = finish(received, tops, parts, 4, width)
    return field.reshape(2, 1, 2, width, width), peak


def solution(mesh):
    in_specs = (P(None, "col", "row", None, None, None), P(), P(), P())
    out_specs = (P("row", "col", None, None, None), P())
    return jax.shard_map(
        on_device, mesh=mesh, in_specs=in_specs, out_specs=out_specs, check_vma=False
    )
```

```python
import math

import jax
import jax.numpy as jnp
import numpy as np
from jax import lax
from jax.experimental import pallas as pl
from jax.experimental.pallas import tpu as pltpu
from jax.sharding import PartitionSpec as P


def spectral_matrix(count):
    gap = (np.arange(count)[:, None] - np.arange(count)[None, :]) % count
    angle = gap.astype(np.float64) * (math.pi / count)
    parity = 1.0 - 2.0 * (gap % 2)
    divisor = np.where(gap == 0, 1.0, np.sin(angle))
    return np.where(gap == 0, 0.0, parity * np.cos(angle) / divisor * (2.0 / count))


def two_halves(matrix):
    high = matrix.astype(np.float32).astype(jnp.bfloat16)
    low = (matrix - high.astype(np.float64)).astype(np.float32).astype(jnp.bfloat16)
    return jnp.asarray(high), jnp.asarray(low)


def split(value):
    high = value.astype(jnp.bfloat16)
    return high, (value - high.astype(jnp.float32)).astype(jnp.bfloat16)


def dot(a, b):
    return jnp.dot(a, b, preferred_element_type=jnp.float32)


def fused_kernel(
    v_ref, high_ref, low_ref, sizes_ref, place_ref, col_ref, out_ref, peak_ref,
    stage, send, in_a, in_x, in_b, aligned, z_high, z_low, y_high, y_low, total, field, shares,
    tops, got, got_tops, ready, ready_tops,
    ends, bounds, source, slab_of,
    in_sems, send_sem, recv_sems, share_send_sems, share_recv_sems,
    peak_send_sems, peak_recv_sems, pair_send_sems, pair_recv_sems, out_sems, out_tops_sem,
):
    fields, rows, planes, width = v_ref.shape
    lanes = send.shape[2]
    parts = lanes
    chunk = send.shape[1] // parts
    per_field = rows // 8
    groups = fields * per_field
    per_chunk = chunk // 8
    chunks_per_field = rows // chunk
    slots = stage.shape[0]
    quarters = total.shape[0]
    half = quarters // 2
    height = total.shape[2]
    pieces = height // lanes
    zblocks, blocks = place_ref.shape
    slabs = col_ref.shape[1]
    depth = rows // 2
    pad = (in_x.shape[0] - parts * rows) // 2
    arrivals = (in_a, in_x, in_b)
    x_section = 1
    row, col = lax.axis_index("row"), lax.axis_index("col")
    me = row * 16 + col
    div, rem = lax.div, lax.rem
    chip, core = row * 8 + div(col, 2), rem(col, 2)
    x, y = div(row, 4) * 2 + rem(div(col, 2), 2), rem(row, 4)
    z = div(col, 4)

    def chip_at(offset):
        there_x = rem(x + div(offset, 16), 4)
        there_y = rem(y + div(offset, 4), 4)
        there_z = rem(z + offset, 4)
        return div(there_x, 2) * 4 + there_y, there_z * 4 + rem(there_x, 2) * 2

    def partner(i):
        offset = rem((i + core * (parts - 2 * i)) * 37, parts)
        to_row, first = chip_at(div(offset, 2))
        return to_row, first + rem(core + offset, 2)

    barrier = pltpu.get_barrier_semaphore()

    def greet(i, _):
        other = rem(me + i, parts)
        pl.semaphore_signal(
            barrier,
            inc=1,
            device_id=(div(other, 16), rem(other, 16)),
            device_id_type=pl.DeviceIdType.MESH,
        )
        return 0

    def loads(f, n):
        at = pl.ds((n - f * per_field) * 8, 8)
        slot = n % slots
        if f == x_section:
            return [pltpu.make_async_copy(v_ref.at[0, at], stage.at[slot], in_sems.at[slot, 0])]
        wide = width // 2
        xs = pl.ds((f // 2) * wide, wide)
        return [
            pltpu.make_async_copy(
                v_ref.at[2 - k, at, :, xs],
                stage.at[slot, :, :, pl.ds(k * wide, wide)],
                in_sems.at[slot, k],
            )
            for k in range(2)
        ]

    def start_load(f, n):
        for copy in loads(f, n):
            copy.start()

    def to_all(copy):
        def one(i, _):
            to_row, to_col = partner(i)
            src, dst, sent, got = copy(to_row * 16 + to_col)
            pltpu.make_async_remote_copy(
                src_ref=src,
                dst_ref=dst,
                send_sem=sent,
                recv_sem=got,
                device_id=(to_row, to_col),
                device_id_type=pl.DeviceIdType.MESH,
            ).start()
            return 0

        lax.fori_loop(1, parts, one, 0)

    def post(j, f):
        arrival = arrivals[f]
        at = pl.ds(pl.multiple_of(pad + me * rows + (j - f * chunks_per_field) * chunk, 8), chunk)
        to_all(
            lambda part: (
                send.at[j, pl.ds(pl.multiple_of(part * chunk, 8), chunk)],
                arrival.at[at],
                send_sem,
                recv_sems.at[f],
            )
        )
        arrival[at, :] = send[j, pl.ds(pl.multiple_of(me * chunk, 8), chunk), :]

    def group(n, f, slope_of, sending=True):
        for copy in loads(f, n):
            copy.wait()
        value = slope_of(stage.at[n % slots])
        for r in range(8):
            piece = value(r)
            stacked = jnp.concatenate(
                [piece[:, q * parts : (q + 1) * parts] for q in range(width // parts)], axis=0
            )
            at = pl.ds((n % per_chunk) * 8 + r, parts, stride=chunk)
            send[n // per_chunk, at, :] = stacked.T

        later = n + slots
        for g in range(f, min(f + 2, fields)):

            @pl.when((later >= g * per_field) & (later < (g + 1) * per_field))
            def _(g=g):
                start_load(g, later)

        if not sending:
            return 0

        if f > 0:

            @pl.when(n == f * per_field)
            def _():
                post(f * chunks_per_field - 1, f - 1)

        @pl.when((n % per_chunk == 0) & (n > (f * per_field if f else per_chunk)))
        def _():
            post(n // per_chunk - 1, f)

        return 0

    def plain(ref):
        return lambda r: ref[r]

    def along_x(ref):
        high, low = split(ref[...].reshape(8 * planes, width))
        slope = dot(high, high_ref[...]) + (dot(high, low_ref[...]) + dot(low, high_ref[...]))
        return lambda r: -slope[r * planes : (r + 1) * planes]

    lax.fori_loop(1, parts, greet, 0)
    for n in range(slots):
        start_load(0, n)
    lax.fori_loop(0, per_chunk, lambda n, _: group(n, 0, plain, False), 0)
    pl.semaphore_wait(barrier, parts - 1)
    post(0, 0)
    for f in range(fields):
        slope_of = along_x if f == x_section else plain
        lax.fori_loop(
            f * per_field if f else per_chunk,
            (f + 1) * per_field,
            lambda n, _, f=f, slope_of=slope_of: group(n, f, slope_of),
            0,
        )
    post(groups // per_chunk - 1, fields - 1)

    end = 0
    for b in range(blocks):
        end = end + sizes_ref[b]
        ends[b] = end
    windows = height // 8

    def window(g, _):
        first = 0
        for b in range(blocks - 1):
            first = first + jnp.where(ends[b] <= 8 * g, 1, 0)
        block = [first, jnp.minimum(first + 1, blocks - 1), jnp.minimum(first + 2, blocks - 1)]
        bounds[2 * g] = ends[block[0]]
        bounds[2 * g + 1] = ends[block[1]]
        skip = [jnp.clip(8 * g - ends[b] + sizes_ref[b], -8, depth - 1) + pad for b in block]

        def on_zblock(c, _):
            for k in range(3):
                place = place_ref[c, block[k]]
                source[c * 3 * windows + 3 * g + k] = (
                    skip[k] + ((place >> 1) * 16 + c) * rows + (place & 1) * depth
                )
            return 0

        lax.fori_loop(0, zblocks, on_zblock, 0)
        return 0

    lax.fori_loop(0, windows, window, 0)

    def holder(i, _):
        zblock, want = i // slabs, i % slabs
        slab = 0
        for h in range(1, slabs):
            slab = jnp.where(col_ref[zblock, h] == want, h, slab)
        slab_of[i] = zblock * planes + 2 * slab
        return 0

    lax.fori_loop(0, zblocks * slabs, holder, 0)

    def arrived(f):
        block = arrivals[f].at[pl.ds(pad, (parts - 1) * rows)]
        pltpu.make_async_copy(block, block, recv_sems.at[f]).wait()

    def align(buffer, c):
        for g in range(windows):
            base = c * 3 * windows + 3 * g
            at = lax.broadcasted_iota(jnp.int32, (8, lanes), 0) + 8 * g
            one, two, three = (buffer[pl.ds(source[base + k], 8), :] for k in range(3))
            value = jnp.where(
                at < bounds[2 * g], one, jnp.where(at < bounds[2 * g + 1], two, three)
            )
            aligned[8 * g : 8 * g + 8, :] = value

    def on_x(c, _):
        align(in_x, c)
        slope = aligned[...].T
        at = pl.ds(pl.multiple_of(c * planes, planes), planes)
        for q in range(quarters):
            total[q, at, :] = slope[q * planes : (q + 1) * planes]
        return 0

    def on_half(h, c):
        align(arrivals[2 * h], c)
        high, low = split(aligned[...].T)
        at = pl.ds(pl.multiple_of(c * planes, planes), planes)
        for q in range(half):
            zs = slice(q * planes, (q + 1) * planes)
            ys = slice((half + q) * planes, (half + q + 1) * planes)
            z_high[half * h + q, at, :] = high[zs]
            z_low[half * h + q, at, :] = low[zs]
            y_high[half * h + q, at, :] = high[ys]
            y_low[half * h + q, at, :] = low[ys]
        return 0

    block_rows = shares.shape[1] // parts
    pitch = got.shape[1] // parts
    mine = pl.ds(pl.multiple_of(me * pitch, 8), block_rows)

    def quarter(h, k):
        q = half * h + k
        along_z = dot(high_ref[...], z_high[q]) + (
            dot(low_ref[...], z_high[q]) + dot(high_ref[...], z_low[q])
        )
        along_y = dot(y_high[q], high_ref[...]) + (
            dot(y_high[q], low_ref[...]) + dot(y_low[q], high_ref[...])
        )
        value = total[q] + (along_z - along_y)
        top = jnp.max(jnp.abs(value), axis=0, keepdims=True)
        for piece in range(pieces):
            along = slice(piece * lanes, (piece + 1) * lanes)
            field[piece * height : (piece + 1) * height, :] = value[:, along]
            tops[h, pl.ds(k * pieces + piece, 1), :] = top[:, along]
        first = pl.multiple_of(k * 4 * pieces, 8)
        for zblock in range(zblocks):
            for holding in range(slabs):
                low_row = slab_of[zblock * slabs + holding]
                target = ((zblock // 2) * slabs + holding) * block_rows + 2 * (zblock % 2)
                for piece in range(pieces):
                    shares[h, pl.ds(first + target + 4 * piece, 2), :] = field[
                        pl.ds(low_row + piece * height, 2), :
                    ]
        return 0

    def give_peaks(h):
        def one(i, _):
            to_row, first = chip_at(rem(i * 37, parts // 2))
            pltpu.make_async_remote_copy(
                src_ref=tops.at[h],
                dst_ref=got_tops.at[h, chip, core],
                send_sem=peak_send_sems.at[h],
                recv_sem=peak_recv_sems.at[h],
                device_id=(to_row, first + core),
                device_id_type=pl.DeviceIdType.MESH,
            ).start()
            return 0

        lax.fori_loop(1, parts // 2, one, 0)
        got_tops[h, chip, core] = tops[h]

    def pair_copy(h):
        held = got_tops.at[h, :, core]
        return pltpu.make_async_remote_copy(
            src_ref=held,
            dst_ref=held,
            send_sem=pair_send_sems.at[h],
            recv_sem=pair_recv_sems.at[h],
            device_id=(row, col + 1 - 2 * core),
            device_id_type=pl.DeviceIdType.MESH,
        )

    def hand_over(h):
        others = got_tops.at[h, pl.ds(0, parts // 2 - 1), 0]
        pltpu.make_async_copy(others, others, peak_send_sems.at[h]).wait()
        pltpu.make_async_copy(others, others, peak_recv_sems.at[h]).wait()
        pair_copy(h).start()

    thick = out_ref.shape[0]

    def put_out(q):
        return pltpu.make_async_copy(
            ready.at[q % half], out_ref.at[:, :, pl.ds(q * lanes, lanes)], out_sems.at[q % half]
        )

    def settle(h):
        others = got.at[h, pl.ds(0, (parts - 1) * block_rows)]
        pltpu.make_async_copy(others, others, share_recv_sems.at[h]).wait()
        for k in range(half):
            if h:
                put_out(half * (h - 1) + k).wait()
            for piece in range(pieces):
                for plane in range(thick):
                    at = pl.ds((k * pieces + piece) * thick + plane, parts, stride=pitch)
                    ready[k, plane, piece * lanes : (piece + 1) * lanes, :] = got[h, at, :].T
            put_out(half * h + k).start()

    def settle_tops():
        for h in range(2):
            pair_copy(h).wait()
            flat = got_tops.at[h].reshape(parts * half * pieces, lanes)
            for k in range(half):
                for piece in range(pieces):
                    at = pl.ds(k * pieces + piece, parts, stride=half * pieces)
                    xs = slice((half * h + k) * lanes, (half * h + k + 1) * lanes)
                    ready_tops[piece * lanes : (piece + 1) * lanes, xs] = flat[at, :].T

    out_tops = pltpu.make_async_copy(ready_tops, peak_ref, out_tops_sem)
    for h in range(2):
        arrived(2 * h)
        lax.fori_loop(0, zblocks, lambda c, _, h=h: on_half(h, c), 0)
        if h == 0:
            arrived(x_section)
            lax.fori_loop(0, zblocks, on_x, 0)
        lax.fori_loop(0, half, lambda k, _, h=h: quarter(h, k), 0)
        give_peaks(h)
        to_all(
            lambda part, h=h: (
                shares.at[h, pl.ds(pl.multiple_of(part * block_rows, 8), block_rows)],
                got.at[h, mine],
                share_send_sems.at[h],
                share_recv_sems.at[h],
            )
        )
        got[h, mine, :] = shares[h, pl.ds(pl.multiple_of(me * block_rows, 8), block_rows), :]

    hand_over(0)
    settle(0)
    hand_over(1)
    settle_tops()
    out_tops.start()
    sent = send.at[:, pl.ds(0, (parts - 1) * chunk)]
    pltpu.make_async_copy(sent, sent, send_sem).wait()
    for h in range(2):
        others = shares.at[h, pl.ds(0, (parts - 1) * block_rows)]
        pltpu.make_async_copy(others, others, share_send_sems.at[h]).wait()
    settle(1)
    for k in range(half):
        put_out(half + k).wait()
    out_tops.wait()


def fused(velocity, high, low, sizes, old_place, new_col, parts):
    fields, rows, planes, width = velocity.shape
    lanes = planes * width // parts
    height = width
    chunk = 24
    quarters = width // parts
    zblocks, blocks = old_place.shape
    block_rows = 32
    vmem = pl.BlockSpec(memory_space=pltpu.VMEM)
    smem = pl.BlockSpec(memory_space=pltpu.SMEM)
    anywhere = pl.BlockSpec(memory_space=pl.ANY)
    arrival = pltpu.VMEM((parts * rows + 16, lanes), jnp.float32)
    operand = pltpu.VMEM((quarters, height, height), jnp.bfloat16)
    return pl.pallas_call(
        fused_kernel,
        in_specs=[anywhere, vmem, vmem, smem, smem, smem],
        out_specs=[anywhere, anywhere],
        out_shape=[
            jax.ShapeDtypeStruct((4, height, width), jnp.float32),
            jax.ShapeDtypeStruct((height, width), jnp.float32),
        ],
        scratch_shapes=[
            pltpu.VMEM((3, 8, planes, width), jnp.float32),
            pltpu.VMEM((fields * rows // chunk, parts * chunk, lanes), jnp.float32),
            arrival,
            arrival,
            arrival,
            pltpu.VMEM((height, lanes), jnp.float32),
            operand,
            operand,
            operand,
            operand,
            pltpu.VMEM((quarters, height, height), jnp.float32),
            pltpu.VMEM((height * height // lanes, lanes), jnp.float32),
            pltpu.VMEM((2, parts * block_rows, lanes), jnp.float32),
            pltpu.VMEM((2, 8, lanes), jnp.float32),
            pltpu.VMEM((2, parts * 40, lanes), jnp.float32),
            pltpu.VMEM((2, parts // 2, 2, 8, lanes), jnp.float32),
            pltpu.VMEM((2, 4, height, lanes), jnp.float32),
            pltpu.VMEM((height, width), jnp.float32),
            pltpu.SMEM((blocks,), jnp.int32),
            pltpu.SMEM((height // 4,), jnp.int32),
            pltpu.SMEM((zblocks * 3 * height // 8,), jnp.int32),
            pltpu.SMEM((zblocks * new_col.shape[1],), jnp.int32),
            pltpu.SemaphoreType.DMA((3, 2)),
            pltpu.SemaphoreType.DMA,
            pltpu.SemaphoreType.DMA((3,)),
        ]
        + [pltpu.SemaphoreType.DMA((2,))] * 7
        + [pltpu.SemaphoreType.DMA],
        compiler_params=pltpu.CompilerParams(
            vmem_limit_bytes=63 << 20, has_side_effects=True, collective_id=0
        ),
        cost_estimate=pl.CostEstimate(
            flops=54 * height**3, bytes_accessed=32 << 20, transcendentals=0
        ),
        name="fused",
    )(velocity, high, low, sizes, old_place, new_col)


def on_device(velocity, y_sizes, old_place, new_col):
    fields, _, places, depth, planes, width = velocity.shape
    parts = lax.axis_size("row") * lax.axis_size("col")
    high, low = two_halves(spectral_matrix(width))
    field, peak = fused(
        velocity.reshape(fields, places * depth, planes, width),
        high,
        low,
        y_sizes,
        old_place,
        new_col,
        parts,
    )
    return field.reshape(2, 1, 2, width, width), peak


def solution(mesh):
    in_specs = (P(None, "col", "row", None, None, None), P(), P(), P())
    out_specs = (P("row", "col", None, None, None), P())
    return jax.shard_map(
        on_device, mesh=mesh, in_specs=in_specs, out_specs=out_specs, check_vma=False
    )
```

```python
import functools
import math

import jax
import jax.numpy as jnp
import numpy as np
from jax import lax
from jax.experimental import pallas as pl
from jax.experimental.pallas import tpu as pltpu
from jax.sharding import PartitionSpec as P


def spectral_matrix(count):
    gap = (np.arange(count)[:, None] - np.arange(count)[None, :]) % count
    angle = gap.astype(np.float64) * (math.pi / count)
    parity = 1.0 - 2.0 * (gap % 2)
    divisor = np.where(gap == 0, 1.0, np.sin(angle))
    return np.where(gap == 0, 0.0, parity * np.cos(angle) / divisor * (2.0 / count))


def two_halves(matrix):
    high = matrix.astype(np.float32).astype(jnp.bfloat16)
    low = (matrix - high.astype(np.float64)).astype(np.float32).astype(jnp.bfloat16)
    return jnp.asarray(high), jnp.asarray(low)


def split(value):
    high = value.astype(jnp.bfloat16)
    return high, (value - high.astype(jnp.float32)).astype(jnp.bfloat16)


def dot(a, b):
    return jnp.dot(a, b, preferred_element_type=jnp.float32)


def fused_kernel(
    v_ref, high_ref, low_ref, sizes_ref, place_ref, col_ref, out_ref, late_ref, peak_ref,
    stage, send, in_a, in_x, in_b, aligned, z_high, z_low, y_high, y_low, total, field, shares,
    tops, got, got_tops, ready, ready_tops,
    ends, bounds, source, slab_of,
    in_sems, send_sem, recv_sems, share_send_sems, share_recv_sems,
    peak_send_sems, peak_recv_sems, pair_send_sems, pair_recv_sems, out_sems, out_tops_sem, own_sem,
):
    fields, rows, planes, width = v_ref.shape
    lanes = send.shape[2]
    parts = lanes
    chunk = send.shape[1] // parts
    per_field = rows // 8
    groups = fields * per_field
    per_chunk = chunk // 8
    chunks_per_field = rows // chunk
    slots = stage.shape[0]
    quarters = total.shape[0]
    half = quarters // 2
    height = total.shape[2]
    pieces = height // lanes
    zblocks, blocks = place_ref.shape
    slabs = col_ref.shape[1]
    depth = rows // 2
    pad = (in_x.shape[0] - parts * rows) // 2
    arrivals = (in_a, in_x, in_b)
    x_section = 1
    row, col = lax.axis_index("row"), lax.axis_index("col")
    me = row * 16 + col
    div, rem = lax.div, lax.rem
    chip, core = row * 8 + div(col, 2), rem(col, 2)
    x, y = div(row, 4) * 2 + rem(div(col, 2), 2), rem(row, 4)
    z = div(col, 4)

    def chip_at(offset):
        there_x = rem(x + div(offset, 16), 4)
        there_y = rem(y + div(offset, 4), 4)
        there_z = rem(z + offset, 4)
        return div(there_x, 2) * 4 + there_y, there_z * 4 + rem(there_x, 2) * 2

    def partner(i):
        offset = rem((i + core * (parts - 2 * i)) * 37, parts)
        to_row, first = chip_at(div(offset, 2))
        return to_row, first + rem(core + offset, 2)

    barrier = pltpu.get_barrier_semaphore()

    def greet(i, _):
        other = rem(me + i, parts)
        pl.semaphore_signal(
            barrier,
            inc=1,
            device_id=(div(other, 16), rem(other, 16)),
            device_id_type=pl.DeviceIdType.MESH,
        )
        return 0

    def loads(f, n):
        at = pl.ds((n - f * per_field) * 8, 8)
        slot = n % slots
        if f == x_section:
            return [pltpu.make_async_copy(v_ref.at[0, at], stage.at[slot], in_sems.at[slot, 0])]
        wide = width // 2
        xs = pl.ds((f // 2) * wide, wide)
        return [
            pltpu.make_async_copy(
                v_ref.at[2 - k, at, :, xs],
                stage.at[slot, :, :, pl.ds(k * wide, wide)],
                in_sems.at[slot, k],
            )
            for k in range(2)
        ]

    def start_load(f, n):
        for copy in loads(f, n):
            copy.start()

    def to_all(copy):
        def one(i, _):
            to_row, to_col = partner(i)
            src, dst, sent, got = copy(to_row * 16 + to_col)
            pltpu.make_async_remote_copy(
                src_ref=src,
                dst_ref=dst,
                send_sem=sent,
                recv_sem=got,
                device_id=(to_row, to_col),
                device_id_type=pl.DeviceIdType.MESH,
            ).start()
            return 0

        lax.fori_loop(1, parts, one, 0)

    def post(j, f):
        arrival = arrivals[f]
        at = pl.ds(pl.multiple_of(pad + me * rows + (j - f * chunks_per_field) * chunk, 8), chunk)
        to_all(
            lambda part: (
                send.at[j, pl.ds(pl.multiple_of(part * chunk, 8), chunk)],
                arrival.at[at],
                send_sem,
                recv_sems.at[f],
            )
        )
        arrival[at, :] = send[j, pl.ds(pl.multiple_of(me * chunk, 8), chunk), :]

    def group(n, f, slope_of, sending=True):
        for copy in loads(f, n):
            copy.wait()
        value = slope_of(stage.at[n % slots])
        for r in range(8):
            piece = value(r)
            stacked = jnp.concatenate(
                [piece[:, q * parts : (q + 1) * parts] for q in range(width // parts)], axis=0
            )
            at = pl.ds((n % per_chunk) * 8 + r, parts, stride=chunk)
            send[n // per_chunk, at, :] = stacked.T

        later = n + slots
        for g in range(f, min(f + 2, fields)):

            @pl.when((later >= g * per_field) & (later < (g + 1) * per_field))
            def _(g=g):
                start_load(g, later)

        if not sending:
            return 0

        if f > 0:

            @pl.when(n == f * per_field)
            def _():
                post(f * chunks_per_field - 1, f - 1)

        @pl.when((n % per_chunk == 0) & (n > (f * per_field if f else per_chunk)))
        def _():
            post(n // per_chunk - 1, f)

        return 0

    def plain(ref):
        return lambda r: ref[r]

    def along_x(ref):
        high, low = split(ref[...].reshape(8 * planes, width))
        slope = dot(high, high_ref[...]) + (dot(high, low_ref[...]) + dot(low, high_ref[...]))
        return lambda r: -slope[r * planes : (r + 1) * planes]

    lax.fori_loop(1, parts, greet, 0)
    for n in range(slots):
        start_load(0, n)
    lax.fori_loop(0, per_chunk, lambda n, _: group(n, 0, plain, False), 0)
    pl.semaphore_wait(barrier, parts - 1)
    post(0, 0)
    for f in range(fields):
        slope_of = along_x if f == x_section else plain
        lax.fori_loop(
            f * per_field if f else per_chunk,
            (f + 1) * per_field,
            lambda n, _, f=f, slope_of=slope_of: group(n, f, slope_of),
            0,
        )
    post(groups // per_chunk - 1, fields - 1)

    end = 0
    for b in range(blocks):
        end = end + sizes_ref[b]
        ends[b] = end
    windows = height // 8

    def window(g, _):
        first = 0
        for b in range(blocks - 1):
            first = first + jnp.where(ends[b] <= 8 * g, 1, 0)
        block = [first, jnp.minimum(first + 1, blocks - 1), jnp.minimum(first + 2, blocks - 1)]
        bounds[2 * g] = ends[block[0]]
        bounds[2 * g + 1] = ends[block[1]]
        skip = [jnp.clip(8 * g - ends[b] + sizes_ref[b], -8, depth - 1) + pad for b in block]

        def on_zblock(c, _):
            for k in range(3):
                place = place_ref[c, block[k]]
                source[c * 3 * windows + 3 * g + k] = (
                    skip[k] + ((place >> 1) * 16 + c) * rows + (place & 1) * depth
                )
            return 0

        lax.fori_loop(0, zblocks, on_zblock, 0)
        return 0

    lax.fori_loop(0, windows, window, 0)

    def holder(i, _):
        zblock, want = i // slabs, i % slabs
        slab = 0
        for h in range(1, slabs):
            slab = jnp.where(col_ref[zblock, h] == want, h, slab)
        slab_of[i] = zblock * planes + 2 * slab
        return 0

    lax.fori_loop(0, zblocks * slabs, holder, 0)

    def arrived(f):
        block = arrivals[f].at[pl.ds(pad, (parts - 1) * rows)]
        pltpu.make_async_copy(block, block, recv_sems.at[f]).wait()

    def align(buffer, c):
        for g in range(windows):
            base = c * 3 * windows + 3 * g
            at = lax.broadcasted_iota(jnp.int32, (8, lanes), 0) + 8 * g
            one, two, three = (buffer[pl.ds(source[base + k], 8), :] for k in range(3))
            value = jnp.where(
                at < bounds[2 * g], one, jnp.where(at < bounds[2 * g + 1], two, three)
            )
            aligned[8 * g : 8 * g + 8, :] = value

    def on_x(c, _):
        align(in_x, c)
        slope = aligned[...].T
        at = pl.ds(pl.multiple_of(c * planes, planes), planes)
        for q in range(quarters):
            total[q, at, :] = slope[q * planes : (q + 1) * planes]
        return 0

    def on_half(h, c):
        align(arrivals[2 * h], c)
        high, low = split(aligned[...].T)
        at = pl.ds(pl.multiple_of(c * planes, planes), planes)
        for q in range(half):
            zs = slice(q * planes, (q + 1) * planes)
            ys = slice((half + q) * planes, (half + q + 1) * planes)
            z_high[half * h + q, at, :] = high[zs]
            z_low[half * h + q, at, :] = low[zs]
            y_high[half * h + q, at, :] = high[ys]
            y_low[half * h + q, at, :] = low[ys]
        return 0

    block_rows = shares.shape[1] // parts
    pitch = got.shape[0] // parts
    landing = (got, late_ref)
    mine = pl.ds(pl.multiple_of(me * pitch, 8), block_rows)

    def quarter(h, k):
        q = half * h + k
        along_z = dot(high_ref[...], z_high[q]) + (
            dot(low_ref[...], z_high[q]) + dot(high_ref[...], z_low[q])
        )
        along_y = dot(y_high[q], high_ref[...]) + (
            dot(y_high[q], low_ref[...]) + dot(y_low[q], high_ref[...])
        )
        value = total[q] + (along_z - along_y)
        top = jnp.max(jnp.abs(value), axis=0, keepdims=True)
        for piece in range(pieces):
            along = slice(piece * lanes, (piece + 1) * lanes)
            field[piece * height : (piece + 1) * height, :] = value[:, along]
            tops[h, pl.ds(k * pieces + piece, 1), :] = top[:, along]
        first = pl.multiple_of(k * 4 * pieces, 8)
        for zblock in range(zblocks):
            for holding in range(slabs):
                low_row = slab_of[zblock * slabs + holding]
                target = ((zblock // 2) * slabs + holding) * block_rows + 2 * (zblock % 2)
                for piece in range(pieces):
                    shares[h, pl.ds(first + target + 4 * piece, 2), :] = field[
                        pl.ds(low_row + piece * height, 2), :
                    ]
        return 0

    def give_peaks(h):
        def one(i, _):
            to_row, first = chip_at(rem(i * 37, parts // 2))
            pltpu.make_async_remote_copy(
                src_ref=tops.at[h],
                dst_ref=got_tops.at[h, chip, core],
                send_sem=peak_send_sems.at[h],
                recv_sem=peak_recv_sems.at[h],
                device_id=(to_row, first + core),
                device_id_type=pl.DeviceIdType.MESH,
            ).start()
            return 0

        lax.fori_loop(1, parts // 2, one, 0)
        got_tops[h, chip, core] = tops[h]

    def pair_copy(h):
        held = got_tops.at[h, :, core]
        return pltpu.make_async_remote_copy(
            src_ref=held,
            dst_ref=held,
            send_sem=pair_send_sems.at[h],
            recv_sem=pair_recv_sems.at[h],
            device_id=(row, col + 1 - 2 * core),
            device_id_type=pl.DeviceIdType.MESH,
        )

    def hand_over(h):
        others = got_tops.at[h, pl.ds(0, parts // 2 - 1), 0]
        pltpu.make_async_copy(others, others, peak_send_sems.at[h]).wait()
        pltpu.make_async_copy(others, others, peak_recv_sems.at[h]).wait()
        pair_copy(h).start()

    thick = out_ref.shape[0]

    def put_out(q):
        return pltpu.make_async_copy(
            ready.at[q], out_ref.at[:, :, pl.ds(q * lanes, lanes)], out_sems.at[q]
        )

    def all_landed(h):
        others = landing[h].at[pl.ds(0, (parts - 1) * block_rows)]
        pltpu.make_async_copy(others, others, share_recv_sems.at[h]).wait()

    def settle_first():
        all_landed(0)
        for k in range(half):
            for piece in range(pieces):
                for plane in range(thick):
                    at = pl.ds((k * pieces + piece) * thick + plane, parts, stride=pitch)
                    ready[k, plane, piece * lanes : (piece + 1) * lanes, :] = got[at, :].T
            put_out(k).start()

    def settle_tops():
        for h in range(2):
            pair_copy(h).wait()
            flat = got_tops.at[h].reshape(parts * half * pieces, lanes)
            for k in range(half):
                for piece in range(pieces):
                    at = pl.ds(k * pieces + piece, parts, stride=half * pieces)
                    xs = slice((half * h + k) * lanes, (half * h + k + 1) * lanes)
                    ready_tops[piece * lanes : (piece + 1) * lanes, xs] = flat[at, :].T

    out_tops = pltpu.make_async_copy(ready_tops, peak_ref, out_tops_sem)
    for h in range(2):
        arrived(2 * h)
        lax.fori_loop(0, zblocks, lambda c, _, h=h: on_half(h, c), 0)
        if h == 0:
            arrived(x_section)
            lax.fori_loop(0, zblocks, on_x, 0)
        lax.fori_loop(0, half, lambda k, _, h=h: quarter(h, k), 0)
        give_peaks(h)
        to_all(
            lambda part, h=h: (
                shares.at[h, pl.ds(pl.multiple_of(part * block_rows, 8), block_rows)],
                landing[h].at[mine],
                share_send_sems.at[h],
                share_recv_sems.at[h],
            )
        )
        kept = pl.ds(pl.multiple_of(me * block_rows, 8), block_rows)
        if h == 0:
            got[mine, :] = shares[h, kept, :]
        else:
            own = pltpu.make_async_copy(shares.at[h, kept], late_ref.at[mine], own_sem)
            own.start()

    hand_over(0)
    settle_first()
    hand_over(1)
    settle_tops()
    out_tops.start()
    sent = send.at[:, pl.ds(0, (parts - 1) * chunk)]
    pltpu.make_async_copy(sent, sent, send_sem).wait()
    for h in range(2):
        others = shares.at[h, pl.ds(0, (parts - 1) * block_rows)]
        pltpu.make_async_copy(others, others, share_send_sems.at[h]).wait()
    for k in range(half):
        put_out(k).wait()
    out_tops.wait()
    own.wait()
    all_landed(1)


def fused(velocity, high, low, sizes, old_place, new_col, parts):
    fields, rows, planes, width = velocity.shape
    lanes = planes * width // parts
    height = width
    chunk = 24
    quarters = width // parts
    zblocks, blocks = old_place.shape
    block_rows = 32
    vmem = pl.BlockSpec(memory_space=pltpu.VMEM)
    smem = pl.BlockSpec(memory_space=pltpu.SMEM)
    anywhere = pl.BlockSpec(memory_space=pl.ANY)
    arrival = pltpu.VMEM((parts * rows + 16, lanes), jnp.float32)
    operand = pltpu.VMEM((quarters, height, height), jnp.bfloat16)
    return pl.pallas_call(
        fused_kernel,
        in_specs=[anywhere, vmem, vmem, smem, smem, smem],
        out_specs=[anywhere, anywhere, anywhere],
        out_shape=[
            jax.ShapeDtypeStruct((4, height, width // 2), jnp.float32),
            jax.ShapeDtypeStruct((parts * 40, lanes), jnp.float32),
            jax.ShapeDtypeStruct((height, width), jnp.float32),
        ],
        scratch_shapes=[
            pltpu.VMEM((3, 8, planes, width), jnp.float32),
            pltpu.VMEM((fields * rows // chunk, parts * chunk, lanes), jnp.float32),
            arrival,
            arrival,
            arrival,
            pltpu.VMEM((height, lanes), jnp.float32),
            operand,
            operand,
            operand,
            operand,
            pltpu.VMEM((quarters, height, height), jnp.float32),
            pltpu.VMEM((height * height // lanes, lanes), jnp.float32),
            pltpu.VMEM((2, parts * block_rows, lanes), jnp.float32),
            pltpu.VMEM((2, 8, lanes), jnp.float32),
            pltpu.VMEM((parts * 40, lanes), jnp.float32),
            pltpu.VMEM((2, parts // 2, 2, 8, lanes), jnp.float32),
            pltpu.VMEM((2, 4, height, lanes), jnp.float32),
            pltpu.VMEM((height, width), jnp.float32),
            pltpu.SMEM((blocks,), jnp.int32),
            pltpu.SMEM((height // 4,), jnp.int32),
            pltpu.SMEM((zblocks * 3 * height // 8,), jnp.int32),
            pltpu.SMEM((zblocks * new_col.shape[1],), jnp.int32),
            pltpu.SemaphoreType.DMA((3, 2)),
            pltpu.SemaphoreType.DMA,
            pltpu.SemaphoreType.DMA((3,)),
        ]
        + [pltpu.SemaphoreType.DMA((2,))] * 7
        + [pltpu.SemaphoreType.DMA] * 2,
        compiler_params=pltpu.CompilerParams(
            vmem_limit_bytes=63 << 20, has_side_effects=True, collective_id=0
        ),
        cost_estimate=pl.CostEstimate(
            flops=54 * height**3, bytes_accessed=32 << 20, transcendentals=0
        ),
        name="fused",
    )(velocity, high, low, sizes, old_place, new_col)


def finish_kernel(first_ref, late_ref, top_ref, out_ref, peak_ref, *, parts):
    plane = pl.program_id(0)
    thick = pl.num_programs(0)
    done, lanes = first_ref.shape[2], late_ref.shape[1]
    pieces = first_ref.shape[1] // lanes
    out_ref[0, :, :done] = first_ref[0]
    peak_ref[...] = top_ref[...]
    for k in range((out_ref.shape[2] - done) // parts):
        for piece in range(pieces):
            start = (k * pieces + piece) * thick + plane
            at = pl.ds(start, parts, stride=late_ref.shape[0] // parts)
            xs = slice(done + k * parts, done + (k + 1) * parts)
            out_ref[0, piece * lanes : (piece + 1) * lanes, xs] = late_ref[at, :].T


def finish(first, late, top, parts):
    thick, height, done = first.shape
    width = top.shape[1]
    tops = pl.BlockSpec((height // thick, width), lambda p: (p, 0))
    return pl.pallas_call(
        functools.partial(finish_kernel, parts=parts),
        grid=(thick,),
        in_specs=[
            pl.BlockSpec((1, height, done), lambda p: (p, 0, 0)),
            pl.BlockSpec(late.shape, lambda p: (0, 0)),
            tops,
        ],
        out_specs=[pl.BlockSpec((1, height, width), lambda p: (p, 0, 0)), tops],
        out_shape=[
            jax.ShapeDtypeStruct((thick, height, width), jnp.float32),
            jax.ShapeDtypeStruct(top.shape, jnp.float32),
        ],
        compiler_params=pltpu.CompilerParams(vmem_limit_bytes=63 << 20),
        cost_estimate=pl.CostEstimate(flops=1 << 20, bytes_accessed=10 << 20, transcendentals=0),
        name="finish",
    )(first, late, top)


def on_device(velocity, y_sizes, old_place, new_col):
    fields, _, places, depth, planes, width = velocity.shape
    parts = lax.axis_size("row") * lax.axis_size("col")
    high, low = two_halves(spectral_matrix(width))
    first, late, peak = fused(
        velocity.reshape(fields, places * depth, planes, width),
        high,
        low,
        y_sizes,
        old_place,
        new_col,
        parts,
    )
    field, peak = finish(first, late, peak, parts)
    return field.reshape(2, 1, 2, width, width), peak


def solution(mesh):
    in_specs = (P(None, "col", "row", None, None, None), P(), P(), P())
    out_specs = (P("row", "col", None, None, None), P())
    return jax.shard_map(
        on_device, mesh=mesh, in_specs=in_specs, out_specs=out_specs, check_vma=False
    )
```

```python
import functools
import math

import jax
import jax.numpy as jnp
import numpy as np
from jax import lax
from jax.experimental import pallas as pl
from jax.experimental.pallas import tpu as pltpu
from jax.sharding import PartitionSpec as P


def spectral_matrix(count):
    gap = (np.arange(count)[:, None] - np.arange(count)[None, :]) % count
    angle = gap.astype(np.float64) * (math.pi / count)
    parity = 1.0 - 2.0 * (gap % 2)
    divisor = np.where(gap == 0, 1.0, np.sin(angle))
    return np.where(gap == 0, 0.0, parity * np.cos(angle) / divisor * (2.0 / count))


def two_halves(matrix):
    high = matrix.astype(np.float32).astype(jnp.bfloat16)
    low = (matrix - high.astype(np.float64)).astype(np.float32).astype(jnp.bfloat16)
    return jnp.asarray(high), jnp.asarray(low)


def split(value):
    high = value.astype(jnp.bfloat16)
    return high, (value - high.astype(jnp.float32)).astype(jnp.bfloat16)


def dot(a, b):
    return jnp.dot(a, b, preferred_element_type=jnp.float32)


def fused_kernel(
    v_ref, high_hbm, low_hbm, sizes_ref, place_ref, col_ref, out_ref, late_ref, peak_ref,
    high_ref, low_ref, stage, send, in_a, in_x, in_b, aligned, z_high, z_low, y_high, y_low, total, field, shares,
    tops, got, got_tops, ready, ready_tops,
    ends, bounds, source, slab_of,
    matrix_sems, in_sems, send_sem, recv_sems, share_send_sems, share_recv_sems,
    peak_send_sems, peak_recv_sems, pair_send_sems, pair_recv_sems, out_sems, out_tops_sem, own_sem,
):
    fields, rows, planes, width = v_ref.shape
    lanes = send.shape[2]
    parts = lanes
    chunk = send.shape[1] // parts
    per_field = rows // 8
    groups = fields * per_field
    per_chunk = chunk // 8
    chunks_per_field = rows // chunk
    slots = stage.shape[0]
    quarters = total.shape[0]
    half = quarters // 2
    height = total.shape[2]
    pieces = height // lanes
    zblocks, blocks = place_ref.shape
    slabs = col_ref.shape[1]
    depth = rows // 2
    pad = (in_x.shape[0] - parts * rows) // 2
    arrivals = (in_a, in_x, in_b)
    x_section = 1
    row, col = lax.axis_index("row"), lax.axis_index("col")
    me = row * 16 + col
    div, rem = lax.div, lax.rem
    chip, core = row * 8 + div(col, 2), rem(col, 2)
    x, y = div(row, 4) * 2 + rem(div(col, 2), 2), rem(row, 4)
    z = div(col, 4)

    def chip_at(offset):
        there_x = rem(x + div(offset, 16), 4)
        there_y = rem(y + div(offset, 4), 4)
        there_z = rem(z + offset, 4)
        return div(there_x, 2) * 4 + there_y, there_z * 4 + rem(there_x, 2) * 2

    def partner(i):
        offset = rem((i + core * (parts - 2 * i)) * 37, parts)
        to_row, first = chip_at(div(offset, 2))
        return to_row, first + rem(core + offset, 2)

    barrier = pltpu.get_barrier_semaphore()

    def greet(i, _):
        other = rem(me + i, parts)
        pl.semaphore_signal(
            barrier,
            inc=1,
            device_id=(div(other, 16), rem(other, 16)),
            device_id_type=pl.DeviceIdType.MESH,
        )
        return 0

    def loads(f, n):
        at = pl.ds((n - f * per_field) * 8, 8)
        slot = n % slots
        if f == x_section:
            return [pltpu.make_async_copy(v_ref.at[0, at], stage.at[slot], in_sems.at[slot, 0])]
        wide = width // 2
        xs = pl.ds((f // 2) * wide, wide)
        return [
            pltpu.make_async_copy(
                v_ref.at[2 - k, at, :, xs],
                stage.at[slot, :, :, pl.ds(k * wide, wide)],
                in_sems.at[slot, k],
            )
            for k in range(2)
        ]

    def start_load(f, n):
        for copy in loads(f, n):
            copy.start()

    def to_all(copy):
        def one(i, _):
            to_row, to_col = partner(i)
            src, dst, sent, got = copy(to_row * 16 + to_col)
            pltpu.make_async_remote_copy(
                src_ref=src,
                dst_ref=dst,
                send_sem=sent,
                recv_sem=got,
                device_id=(to_row, to_col),
                device_id_type=pl.DeviceIdType.MESH,
            ).start()
            return 0

        lax.fori_loop(1, parts, one, 0)

    def post(j, f):
        arrival = arrivals[f]
        at = pl.ds(pl.multiple_of(pad + me * rows + (j - f * chunks_per_field) * chunk, 8), chunk)
        to_all(
            lambda part: (
                send.at[j, pl.ds(pl.multiple_of(part * chunk, 8), chunk)],
                arrival.at[at],
                send_sem,
                recv_sems.at[f],
            )
        )
        arrival[at, :] = send[j, pl.ds(pl.multiple_of(me * chunk, 8), chunk), :]

    def group(n, f, slope_of, sending=True):
        for copy in loads(f, n):
            copy.wait()
        value = slope_of(stage.at[n % slots])
        for r in range(8):
            piece = value(r)
            stacked = jnp.concatenate(
                [piece[:, q * parts : (q + 1) * parts] for q in range(width // parts)], axis=0
            )
            at = pl.ds((n % per_chunk) * 8 + r, parts, stride=chunk)
            send[n // per_chunk, at, :] = stacked.T

        later = n + slots
        for g in range(f, min(f + 2, fields)):

            @pl.when((later >= g * per_field) & (later < (g + 1) * per_field))
            def _(g=g):
                start_load(g, later)

        if not sending:
            return 0

        if f > 0:

            @pl.when(n == f * per_field)
            def _():
                post(f * chunks_per_field - 1, f - 1)

        @pl.when((n % per_chunk == 0) & (n > (f * per_field if f else per_chunk)))
        def _():
            post(n // per_chunk - 1, f)

        return 0

    def plain(ref):
        return lambda r: ref[r]

    def along_x(ref):
        high, low = split(ref[...].reshape(8 * planes, width))
        slope = dot(high, high_ref[...]) + (dot(high, low_ref[...]) + dot(low, high_ref[...]))
        return lambda r: -slope[r * planes : (r + 1) * planes]

    for n in range(slots):
        start_load(0, n)
    matrix = [
        pltpu.make_async_copy(high_hbm, high_ref, matrix_sems.at[0]),
        pltpu.make_async_copy(low_hbm, low_ref, matrix_sems.at[1]),
    ]
    for copy in matrix:
        copy.start()
    lax.fori_loop(1, parts, greet, 0)
    lax.fori_loop(0, per_chunk, lambda n, _: group(n, 0, plain, False), 0)
    pl.semaphore_wait(barrier, parts - 1)
    post(0, 0)
    for f in range(fields):
        slope_of = along_x if f == x_section else plain
        if f == x_section:
            for copy in matrix:
                copy.wait()
        lax.fori_loop(
            f * per_field if f else per_chunk,
            (f + 1) * per_field,
            lambda n, _, f=f, slope_of=slope_of: group(n, f, slope_of),
            0,
        )
    post(groups // per_chunk - 1, fields - 1)

    end = 0
    for b in range(blocks):
        end = end + sizes_ref[b]
        ends[b] = end
    windows = height // 8

    def window(g, _):
        first = 0
        for b in range(blocks - 1):
            first = first + jnp.where(ends[b] <= 8 * g, 1, 0)
        block = [first, jnp.minimum(first + 1, blocks - 1), jnp.minimum(first + 2, blocks - 1)]
        bounds[2 * g] = ends[block[0]]
        bounds[2 * g + 1] = ends[block[1]]
        skip = [jnp.clip(8 * g - ends[b] + sizes_ref[b], -8, depth - 1) + pad for b in block]

        def on_zblock(c, _):
            for k in range(3):
                place = place_ref[c, block[k]]
                source[c * 3 * windows + 3 * g + k] = (
                    skip[k] + ((place >> 1) * 16 + c) * rows + (place & 1) * depth
                )
            return 0

        lax.fori_loop(0, zblocks, on_zblock, 0)
        return 0

    lax.fori_loop(0, windows, window, 0)

    def holder(i, _):
        zblock, want = i // slabs, i % slabs
        slab = 0
        for h in range(1, slabs):
            slab = jnp.where(col_ref[zblock, h] == want, h, slab)
        slab_of[i] = zblock * planes + 2 * slab
        return 0

    lax.fori_loop(0, zblocks * slabs, holder, 0)

    def arrived(f):
        block = arrivals[f].at[pl.ds(pad, (parts - 1) * rows)]
        pltpu.make_async_copy(block, block, recv_sems.at[f]).wait()

    def align(buffer, c):
        for g in range(windows):
            base = c * 3 * windows + 3 * g
            at = lax.broadcasted_iota(jnp.int32, (8, lanes), 0) + 8 * g
            one, two, three = (buffer[pl.ds(source[base + k], 8), :] for k in range(3))
            value = jnp.where(
                at < bounds[2 * g], one, jnp.where(at < bounds[2 * g + 1], two, three)
            )
            aligned[8 * g : 8 * g + 8, :] = value

    def on_x(c, _):
        align(in_x, c)
        slope = aligned[...].T
        at = pl.ds(pl.multiple_of(c * planes, planes), planes)
        for q in range(quarters):
            total[q, at, :] = slope[q * planes : (q + 1) * planes]
        return 0

    def on_half(h, c):
        align(arrivals[2 * h], c)
        high, low = split(aligned[...].T)
        at = pl.ds(pl.multiple_of(c * planes, planes), planes)
        for q in range(half):
            zs = slice(q * planes, (q + 1) * planes)
            ys = slice((half + q) * planes, (half + q + 1) * planes)
            z_high[half * h + q, at, :] = high[zs]
            z_low[half * h + q, at, :] = low[zs]
            y_high[half * h + q, at, :] = high[ys]
            y_low[half * h + q, at, :] = low[ys]
        return 0

    block_rows = shares.shape[1] // parts
    pitch = got.shape[0] // parts
    landing = (got, late_ref)
    mine = pl.ds(pl.multiple_of(me * pitch, 8), block_rows)

    def quarter(h, k):
        q = half * h + k
        along_z = dot(high_ref[...], z_high[q]) + (
            dot(low_ref[...], z_high[q]) + dot(high_ref[...], z_low[q])
        )
        along_y = dot(y_high[q], high_ref[...]) + (
            dot(y_high[q], low_ref[...]) + dot(y_low[q], high_ref[...])
        )
        value = total[q] + (along_z - along_y)
        top = jnp.max(jnp.abs(value), axis=0, keepdims=True)
        for piece in range(pieces):
            along = slice(piece * lanes, (piece + 1) * lanes)
            field[piece * height : (piece + 1) * height, :] = value[:, along]
            tops[h, pl.ds(k * pieces + piece, 1), :] = top[:, along]
        first = pl.multiple_of(k * 4 * pieces, 8)
        for zblock in range(zblocks):
            for holding in range(slabs):
                low_row = slab_of[zblock * slabs + holding]
                target = ((zblock // 2) * slabs + holding) * block_rows + 2 * (zblock % 2)
                for piece in range(pieces):
                    shares[h, pl.ds(first + target + 4 * piece, 2), :] = field[
                        pl.ds(low_row + piece * height, 2), :
                    ]
        return 0

    def give_peaks(h):
        def one(i, _):
            to_row, first = chip_at(rem(i * 37, parts // 2))
            pltpu.make_async_remote_copy(
                src_ref=tops.at[h],
                dst_ref=got_tops.at[h, chip, core],
                send_sem=peak_send_sems.at[h],
                recv_sem=peak_recv_sems.at[h],
                device_id=(to_row, first + core),
                device_id_type=pl.DeviceIdType.MESH,
            ).start()
            return 0

        lax.fori_loop(1, parts // 2, one, 0)
        got_tops[h, chip, core] = tops[h]

    def pair_copy(h):
        held = got_tops.at[h, :, core]
        return pltpu.make_async_remote_copy(
            src_ref=held,
            dst_ref=held,
            send_sem=pair_send_sems.at[h],
            recv_sem=pair_recv_sems.at[h],
            device_id=(row, col + 1 - 2 * core),
            device_id_type=pl.DeviceIdType.MESH,
        )

    def hand_over(h):
        others = got_tops.at[h, pl.ds(0, parts // 2 - 1), 0]
        pltpu.make_async_copy(others, others, peak_send_sems.at[h]).wait()
        pltpu.make_async_copy(others, others, peak_recv_sems.at[h]).wait()
        pair_copy(h).start()

    thick = out_ref.shape[0]

    def put_out(q):
        return pltpu.make_async_copy(
            ready.at[q], out_ref.at[:, :, pl.ds(q * lanes, lanes)], out_sems.at[q]
        )

    def all_landed(h):
        others = landing[h].at[pl.ds(0, (parts - 1) * block_rows)]
        pltpu.make_async_copy(others, others, share_recv_sems.at[h]).wait()

    def settle_first():
        all_landed(0)
        for k in range(half):
            for piece in range(pieces):
                for plane in range(thick):
                    at = pl.ds((k * pieces + piece) * thick + plane, parts, stride=pitch)
                    ready[k, plane, piece * lanes : (piece + 1) * lanes, :] = got[at, :].T
            put_out(k).start()

    def settle_tops():
        for h in range(2):
            pair_copy(h).wait()
            flat = got_tops.at[h].reshape(parts * half * pieces, lanes)
            for k in range(half):
                for piece in range(pieces):
                    at = pl.ds(k * pieces + piece, parts, stride=half * pieces)
                    xs = slice((half * h + k) * lanes, (half * h + k + 1) * lanes)
                    ready_tops[piece * lanes : (piece + 1) * lanes, xs] = flat[at, :].T

    out_tops = pltpu.make_async_copy(ready_tops, peak_ref, out_tops_sem)
    for h in range(2):
        arrived(2 * h)
        lax.fori_loop(0, zblocks, lambda c, _, h=h: on_half(h, c), 0)
        if h == 0:
            arrived(x_section)
            lax.fori_loop(0, zblocks, on_x, 0)
        lax.fori_loop(0, half, lambda k, _, h=h: quarter(h, k), 0)
        give_peaks(h)
        to_all(
            lambda part, h=h: (
                shares.at[h, pl.ds(pl.multiple_of(part * block_rows, 8), block_rows)],
                landing[h].at[mine],
                share_send_sems.at[h],
                share_recv_sems.at[h],
            )
        )
        kept = pl.ds(pl.multiple_of(me * block_rows, 8), block_rows)
        if h == 0:
            got[mine, :] = shares[h, kept, :]
        else:
            own = pltpu.make_async_copy(shares.at[h, kept], late_ref.at[mine], own_sem)
            own.start()

    hand_over(0)
    settle_first()
    hand_over(1)
    settle_tops()
    out_tops.start()
    sent = send.at[:, pl.ds(0, (parts - 1) * chunk)]
    pltpu.make_async_copy(sent, sent, send_sem).wait()
    for h in range(2):
        others = shares.at[h, pl.ds(0, (parts - 1) * block_rows)]
        pltpu.make_async_copy(others, others, share_send_sems.at[h]).wait()
    for k in range(half):
        put_out(k).wait()
    out_tops.wait()
    own.wait()
    all_landed(1)


def fused(velocity, high, low, sizes, old_place, new_col, parts):
    fields, rows, planes, width = velocity.shape
    lanes = planes * width // parts
    height = width
    chunk = 24
    quarters = width // parts
    zblocks, blocks = old_place.shape
    block_rows = 32
    smem = pl.BlockSpec(memory_space=pltpu.SMEM)
    anywhere = pl.BlockSpec(memory_space=pl.ANY)
    arrival = pltpu.VMEM((parts * rows + 16, lanes), jnp.float32)
    operand = pltpu.VMEM((quarters, height, height), jnp.bfloat16)
    return pl.pallas_call(
        fused_kernel,
        in_specs=[anywhere, anywhere, anywhere, smem, smem, smem],
        out_specs=[anywhere, anywhere, anywhere],
        out_shape=[
            jax.ShapeDtypeStruct((4, height, width // 2), jnp.float32),
            jax.ShapeDtypeStruct((parts * 40, lanes), jnp.float32),
            jax.ShapeDtypeStruct((height, width), jnp.float32),
        ],
        scratch_shapes=[
            pltpu.VMEM((height, height), jnp.bfloat16),
            pltpu.VMEM((height, height), jnp.bfloat16),
            pltpu.VMEM((3, 8, planes, width), jnp.float32),
            pltpu.VMEM((fields * rows // chunk, parts * chunk, lanes), jnp.float32),
            arrival,
            arrival,
            arrival,
            pltpu.VMEM((height, lanes), jnp.float32),
            operand,
            operand,
            operand,
            operand,
            pltpu.VMEM((quarters, height, height), jnp.float32),
            pltpu.VMEM((height * height // lanes, lanes), jnp.float32),
            pltpu.VMEM((2, parts * block_rows, lanes), jnp.float32),
            pltpu.VMEM((2, 8, lanes), jnp.float32),
            pltpu.VMEM((parts * 40, lanes), jnp.float32),
            pltpu.VMEM((2, parts // 2, 2, 8, lanes), jnp.float32),
            pltpu.VMEM((2, 4, height, lanes), jnp.float32),
            pltpu.VMEM((height, width), jnp.float32),
            pltpu.SMEM((blocks,), jnp.int32),
            pltpu.SMEM((height // 4,), jnp.int32),
            pltpu.SMEM((zblocks * 3 * height // 8,), jnp.int32),
            pltpu.SMEM((zblocks * new_col.shape[1],), jnp.int32),
            pltpu.SemaphoreType.DMA((2,)),
            pltpu.SemaphoreType.DMA((3, 2)),
            pltpu.SemaphoreType.DMA,
            pltpu.SemaphoreType.DMA((3,)),
        ]
        + [pltpu.SemaphoreType.DMA((2,))] * 7
        + [pltpu.SemaphoreType.DMA] * 2,
        compiler_params=pltpu.CompilerParams(
            vmem_limit_bytes=63 << 20, has_side_effects=True, collective_id=0
        ),
        cost_estimate=pl.CostEstimate(
            flops=54 * height**3, bytes_accessed=32 << 20, transcendentals=0
        ),
        name="fused",
    )(velocity, high, low, sizes, old_place, new_col)


def finish_kernel(first_ref, late_ref, top_ref, out_ref, peak_ref, *, parts):
    plane = pl.program_id(0)
    thick = pl.num_programs(0)
    done, lanes = first_ref.shape[2], late_ref.shape[1]
    pieces = first_ref.shape[1] // lanes
    out_ref[0, :, :done] = first_ref[0]
    peak_ref[...] = top_ref[...]
    for k in range((out_ref.shape[2] - done) // parts):
        for piece in range(pieces):
            start = (k * pieces + piece) * thick + plane
            at = pl.ds(start, parts, stride=late_ref.shape[0] // parts)
            xs = slice(done + k * parts, done + (k + 1) * parts)
            out_ref[0, piece * lanes : (piece + 1) * lanes, xs] = late_ref[at, :].T


def finish(first, late, top, parts):
    thick, height, done = first.shape
    width = top.shape[1]
    tops = pl.BlockSpec((height // thick, width), lambda p: (p, 0))
    return pl.pallas_call(
        functools.partial(finish_kernel, parts=parts),
        grid=(thick,),
        in_specs=[
            pl.BlockSpec((1, height, done), lambda p: (p, 0, 0)),
            pl.BlockSpec(late.shape, lambda p: (0, 0)),
            tops,
        ],
        out_specs=[pl.BlockSpec((1, height, width), lambda p: (p, 0, 0)), tops],
        out_shape=[
            jax.ShapeDtypeStruct((thick, height, width), jnp.float32),
            jax.ShapeDtypeStruct(top.shape, jnp.float32),
        ],
        compiler_params=pltpu.CompilerParams(vmem_limit_bytes=63 << 20),
        cost_estimate=pl.CostEstimate(flops=1 << 20, bytes_accessed=10 << 20, transcendentals=0),
        name="finish",
    )(first, late, top)


def on_device(velocity, y_sizes, old_place, new_col):
    fields, _, places, depth, planes, width = velocity.shape
    parts = lax.axis_size("row") * lax.axis_size("col")
    high, low = two_halves(spectral_matrix(width))
    first, late, peak = fused(
        velocity.reshape(fields, places * depth, planes, width),
        high,
        low,
        y_sizes,
        old_place,
        new_col,
        parts,
    )
    field, peak = finish(first, late, peak, parts)
    return field.reshape(2, 1, 2, width, width), peak


def solution(mesh):
    in_specs = (P(None, "col", "row", None, None, None), P(), P(), P())
    out_specs = (P("row", "col", None, None, None), P())
    return jax.shard_map(
        on_device, mesh=mesh, in_specs=in_specs, out_specs=out_specs, check_vma=False
    )
```
